512 devices in a mesh: lat: 32 (over z, x), lon: 16 (over y, core).
Axes of the slice: x: 4, y: 8, z: 8, core: 2. Of those that a mesh axis runs over, the one named last changes fastest.
Arguments:
- state_init: float32 [16, 1048576], P(None, ('lat', 'lon')), may hold values from -6 to 6
- tangent_init: float32 [16, 1048576], P(None, ('lat', 'lon')), may hold values from -6 to 6
- coef_blocks: bfloat16 [8192, 6, 128, 128], P(('lat', 'lon')), may hold values from -0.21875 to 0.21875
- column_lists: int32 [8192, 6], P(('lat', 'lon')), may hold values from 0 to 24, as said below
- send_lists: int32 [512, 4, 2], P(('lat', 'lon')), may hold values from 0 to 15, as said below
- implicit_blocks: bfloat16 [8192, 128, 128], P(('lat', 'lon')), may hold values from -0.5 to 0.5
- uptake_rate: float32 [1048576], P(('lat', 'lon')), may hold values from 0.5 to 4
- coupling: float32 [16, 16], replicated, may hold values from -1.5 to 1.5
- region_map: int32 [1048576], P(('lat', 'lon')), may hold values from 0 to 4095, as said below
- coarse_inverse: float32 [4096, 4096], P(('lat', 'lon')), may hold values from -0.005859375 to 0.005859375
Outputs:
- final_state: float32 [16, 1048576], P(None, ('lat', 'lon'))
- preconditioned: float32 [16, 1048576], P(None, ('lat', 'lon'))
The draws below stay inside these ranges and needn't reach their ends.
Inputs may be any that keep to these rules, and one draw needn't show every extreme that they name: `column_lists`: entry 0 of row block b's list is b's own index within its tile; entries 1 to 4 lie in the blocks from the lower lat, higher lat, lower lon and higher lon neighbours in that order; the rest are own blocks or 24, the zero block. `send_lists`: indices of the sending tile's own row blocks. `region_map`: region c is owned by tile c // 8; a row's region is owned by its own tile or by one of its two lon neighbours (wrapping).
All inputs are finite; a program needn't handle non-finite values.
Results may differ from the reference program's by a relative error of at most 0.0064.
Values may be sent and summed in bfloat16 or wider, within the bound.
A program may use at most 64 MiB of HBM per device.

```python
import math
import jax
import jax.numpy as jnp
from jax import lax

NT = 16
BLOCK = 128
RB = 16
K = 6
HB = 2
STEPS = 2
REG_DEV = 8
ROWS = 1048576
BLOCKS = 8192
NC = 4096
N_LAT = 32
N_LON = 16


def draw_column_lists(key, part):
    block_ids = jnp.arange(BLOCKS, dtype=jnp.int32) % RB
    offset = jax.random.randint(jax.random.fold_in(key, 11), (BLOCKS, 1), 0, HB)
    sides = RB + jnp.arange(4, dtype=jnp.int32)[None, :] * HB + (block_ids[:, None] + offset) % HB
    extra = jax.random.randint(jax.random.fold_in(key, 12), (BLOCKS, K - 5), 0, RB + 1)
    extra = jnp.where(extra == RB, RB + 4 * HB, extra)
    return jnp.concatenate([block_ids[:, None], sides, extra], axis=1).astype(jnp.int32)


def draw_send_lists(key, part):
    return jax.random.randint(jax.random.fold_in(key, 21), (N_LAT * N_LON, 4, HB), 0, RB).astype(jnp.int32)


def draw_region_map(key, part):
    rows_all = N_LAT * N_LON * RB * BLOCK
    tile = jnp.arange(rows_all, dtype=jnp.int32) // (RB * BLOCK)
    lat_pos = tile // N_LON
    lon_pos = tile % N_LON
    select = jax.random.randint(jax.random.fold_in(key, 31), (rows_all,), 0, 10)
    step_lon = jnp.where(select == 0, -1, jnp.where(select == 1, 1, 0))
    owner = lat_pos * N_LON + (lon_pos + step_lon + N_LON) % N_LON
    offset = jax.random.randint(jax.random.fold_in(key, 32), (rows_all,), 0, REG_DEV)
    return (owner * REG_DEV + offset).astype(jnp.int32)


def shard_levels(stream_key, shape, split, smallest, largest):
    level = 1.0
    for axis_at, shards_of in split:
        draws = jax.random.uniform(jax.random.fold_in(jax.random.fold_in(stream_key, 6), axis_at), (shards_of,), jnp.float32, smallest / len(split), largest / len(split))
        level = level * jnp.repeat(jnp.exp(draws), shape[axis_at] // shards_of).reshape((-1,) + (1,) * (len(shape) - 1 - axis_at))
    return level


def scatter_about(stream_key, extent, spread, most, shards=(), kind=jnp.bfloat16):
    factor_of = shard_levels(stream_key, extent, shards, -0.22, 0.18) if shards else 1.0
    entries = jax.random.normal(stream_key, extent, jnp.float32) * spread * factor_of
    return jnp.minimum(jnp.maximum(entries, -most), most).astype(kind)


def setup_inputs(seed: int = 0) -> dict:
    keys = jax.random.split(jax.random.key(seed), 11)
    state_init = scatter_about(keys[0], (NT, ROWS), 1.0, 6.0, ((1, 512),), jnp.float32)
    tangent_init = scatter_about(keys[1], (NT, ROWS), 1.0, 6.0, ((1, 512),), jnp.float32)
    coef_blocks = scatter_about(keys[2], (BLOCKS, K, BLOCK, BLOCK), (BLOCK * K) ** -0.5, 0.21875, ((0, 512),))
    column_lists = draw_column_lists(jax.random.fold_in(keys[10], 71), 0)
    send_lists = draw_send_lists(jax.random.fold_in(keys[10], 71), 0)
    implicit_blocks = scatter_about(keys[5], (BLOCKS, BLOCK, BLOCK), BLOCK ** -0.5, 0.5, ((0, 512),))
    uptake_rate = jnp.clip(jnp.exp(math.log(4.0) - 2.0794415 * jax.random.uniform(keys[6], (ROWS,), jnp.float32) ** shard_levels(keys[6], (ROWS,), ((0, 512),), -0.2, 0.2)), 0.5, 4.0)
    coupling = scatter_about(keys[7], (NT, NT), NT ** -0.5, 1.5, (), jnp.float32)
    region_map = draw_region_map(jax.random.fold_in(keys[10], 71), 0)
    coarse_inverse = scatter_about(keys[9], (NC, NC), (RB * BLOCK * N_LAT * N_LON) ** -0.5, 0.005859375, ((0, 512),), jnp.float32)
    return {"state_init": state_init, "tangent_init": tangent_init, "coef_blocks": coef_blocks, "column_lists": column_lists, "send_lists": send_lists, "implicit_blocks": implicit_blocks, "uptake_rate": uptake_rate, "coupling": coupling, "region_map": region_map, "coarse_inverse": coarse_inverse}


step_length = 0.5


def readable_blocks(rounded, send_lists):
    channels = rounded.shape[0]
    tiles = rounded.reshape(channels, N_LAT, N_LON, RB, BLOCK)
    sends = send_lists.reshape(N_LAT, N_LON, 4 * HB)
    lat_ids = jnp.arange(N_LAT)[:, None, None]
    lon_ids = jnp.arange(N_LON)[None, :, None]
    picked = tiles[:, lat_ids, lon_ids, sends].reshape(channels, N_LAT, N_LON, 4, HB, BLOCK)
    zero_row = jnp.zeros_like(picked[:, :1, :, 0])
    from_below = jnp.concatenate([zero_row, picked[:, :-1, :, 0]], axis=1)
    from_above = jnp.concatenate([picked[:, 1:, :, 1], zero_row], axis=1)
    from_west = jnp.roll(picked[:, :, :, 2], 1, axis=2)
    from_east = jnp.roll(picked[:, :, :, 3], -1, axis=2)
    empty = jnp.zeros((channels, N_LAT, N_LON, 1, BLOCK), rounded.dtype)
    return jnp.concatenate([tiles, from_below, from_above, from_west, from_east, empty], axis=3)


def transport(readable, column_lists, coef_blocks):
    lists = column_lists.reshape(N_LAT, N_LON, RB, K)
    coefs = coef_blocks.reshape(N_LAT, N_LON, RB, K, BLOCK, BLOCK)
    lon_ids = jnp.arange(N_LON)[:, None, None]

    def one_lat(items):
        ext_lat, list_lat, coef_lat = items
        gathered = ext_lat[:, lon_ids, list_lat]
        return jnp.einsum("cobkp,obkpq->cobq", gathered.astype(jnp.float32), coef_lat.astype(jnp.float32), precision=lax.Precision.HIGHEST)

    moved = lax.map(one_lat, (jnp.moveaxis(readable, 1, 0), lists, coefs))
    moved = jnp.moveaxis(moved, 0, 1)
    return moved.reshape(readable.shape[0], ROWS)


def reference(state_init, tangent_init, coef_blocks, column_lists, send_lists, implicit_blocks, uptake_rate, coupling, region_map, coarse_inverse):
    state = state_init
    tangent = tangent_init
    channels = 2 * NT
    for sweep_index in range(STEPS):
        stacked = jnp.concatenate([state, tangent], axis=0)
        rounded = stacked.astype(jnp.bfloat16)
        readable = readable_blocks(rounded, send_lists)
        moved = transport(readable, column_lists, coef_blocks)
        squared = state * state
        denom = 1.0 + squared
        uptake = uptake_rate * state / denom
        slope = uptake_rate * (1.0 - squared) / (denom * denom) * tangent
        sources = jnp.dot(coupling, jnp.concatenate([uptake, slope], axis=1), precision=lax.Precision.HIGHEST, preferred_element_type=jnp.float32)
        sources = jnp.concatenate([sources[:, :ROWS], sources[:, ROWS:]], axis=0)
        explicit = (stacked + moved + step_length * sources).astype(jnp.bfloat16)
        shaped = explicit.reshape(channels, BLOCKS, BLOCK).astype(jnp.float32)
        implicit = jnp.einsum("cbp,bpq->cbq", shaped, implicit_blocks.astype(jnp.float32), precision=lax.Precision.HIGHEST)
        implicit = implicit.reshape(channels, ROWS)
        state = implicit[:NT]
        tangent = implicit[NT:]
    residual = tangent - tangent_init
    totals = jax.ops.segment_sum(residual.T, region_map, num_segments=NC).T
    values = jnp.dot(totals, coarse_inverse.T, precision=lax.Precision.HIGHEST, preferred_element_type=jnp.float32)
    preconditioned = residual + jnp.take(values, region_map, axis=1)
    return state, preconditioned
```

```python
import jax
import jax.numpy as jnp
from jax import lax
from jax.experimental import pallas as pl
from jax.experimental.pallas import tpu as pltpu
from jax.sharding import Mesh
from jax.sharding import PartitionSpec as P

NT = 16
STEPS = 2
REG_DEV = 8
RB = 16
K = 6
HB = 2
BLOCK = 128
STEP_LENGTH = 0.5
AXES = ("z", "x", "y", "c")
NZ, NX, NY, NCORE = 8, 4, 8, 2
N_LAT = NZ * NX
N_LON = NY * NCORE
MESH = pl.DeviceIdType.MESH
F32 = jnp.float32
BF16 = jnp.bfloat16


def ring_hops(d, n):
    return min(d, n - d)


LON_PEERS = sorted(
    ((dy, dc) for dy in range(NY) for dc in range(NCORE) if (dy, dc) != (0, 0)),
    key=lambda p: -ring_hops(p[0], NY),
)
LAT_PEERS = sorted(
    ((dz, dx) for dz in range(NZ) for dx in range(NX) if (dz, dx) != (0, 0)),
    key=lambda p: -(ring_hops(p[0], NZ) + ring_hops(p[1], NX)),
)


def kernel(
    state_hbm,
    tangent_hbm,
    coef_hbm,
    lists_hbm,
    sends_hbm,
    implicit_hbm,
    rate_hbm,
    coupling_hbm,
    region_hbm,
    coarse_hbm,
    state_out,
    precond_out,
    state0,
    tang0,
    coef,
    impl,
    rate,
    coup,
    region,
    crow_own,
    crow_low,
    crow_high,
    lists,
    sends,
    own_0,
    own_1,
    rims_0,
    rims_1,
    rims_2,
    rims_3,
    rims_4,
    rims_5,
    rims_6,
    rims_7,
    picks,
    acc,
    stk,
    onehot_t,
    onehot,
    coarse_w,
    tile_lon,
    lon_buf,
    tile_lat,
    lat_buf,
    load_sem,
    rim_send,
    rim_recv,
    crow_send,
    crow_recv,
    lon_send,
    lon_recv,
    lat_send,
    lat_recv,
):
    z, x = lax.axis_index("z"), lax.axis_index("x")
    y, c = lax.axis_index("y"), lax.axis_index("c")
    lat = z * NX + x
    lon = y * NCORE + c
    owns = (own_0, own_1)
    rims = ((rims_0, rims_1, rims_2, rims_3), (rims_4, rims_5, rims_6, rims_7))

    def at_lat(v):
        return (v // NX, v % NX, y, c)

    def at_lon(v):
        return (z, x, v // NCORE, v % NCORE)

    def lon_peer(dy, dc):
        return (z, x, (y + dy) % NY, (c + dc) % NCORE)

    def lat_peer(dz, dx):
        return ((z + dz) % NZ, (x + dx) % NX, y, c)

    barrier = pltpu.get_barrier_semaphore()
    for p in LAT_PEERS:
        pl.semaphore_signal(barrier, inc=1, device_id=lat_peer(*p), device_id_type=MESH)
    for p in LON_PEERS:
        pl.semaphore_signal(barrier, inc=1, device_id=lon_peer(*p), device_id_type=MESH)

    pairs = (
        (sends_hbm, sends),
        (state_hbm, state0),
        (tangent_hbm, tang0),
        (lists_hbm, lists),
        (rate_hbm, rate),
        (coupling_hbm, coup),
        (region_hbm, region),
        (coef_hbm, coef),
        (implicit_hbm, impl),
        (coarse_hbm, crow_own),
    )
    loads = [pltpu.make_async_copy(a, b, load_sem.at[i]) for i, (a, b) in enumerate(pairs)]
    for load in loads:
        load.start()

    def cols(b):
        return slice(b * BLOCK, (b + 1) * BLOCK)

    def rim_copies(s):
        below, above = (lat + N_LAT - 1) % N_LAT, (lat + 1) % N_LAT
        west, east = (lon + N_LON - 1) % N_LON, (lon + 1) % N_LON
        targets = (at_lat(above), at_lat(below), at_lon(east), at_lon(west))
        return [
            pltpu.make_async_remote_copy(
                src_ref=picks.at[s, d],
                dst_ref=rims[s][d],
                send_sem=rim_send.at[s, d],
                recv_sem=rim_recv.at[s, d],
                device_id=targets[d],
                device_id_type=MESH,
            )
            for d in range(4)
        ]

    def send_rims(s):
        for d in range(4):
            for h in range(HB):
                picks[s, d, h] = owns[s][sends[0, h, d]]
        copies = rim_copies(s)

        @pl.when(lat < N_LAT - 1)
        def _():
            copies[0].start()

        @pl.when(lat > 0)
        def _():
            copies[1].start()

        copies[2].start()
        copies[3].start()

    def await_rims(s):
        copies = rim_copies(s)

        @pl.when(lat > 0)
        def _():
            copies[0].wait_recv()

        @pl.when(lat < N_LAT - 1)
        def _():
            copies[1].wait_recv()

        copies[2].wait_recv()
        copies[3].wait_recv()

    def await_rim_sends(s):
        copies = rim_copies(s)

        @pl.when(lat < N_LAT - 1)
        def _():
            copies[0].wait_send()

        @pl.when(lat > 0)
        def _():
            copies[1].wait_send()

        copies[2].wait_send()
        copies[3].wait_send()

    zero_block = jnp.zeros((2 * NT, BLOCK), BF16)
    for s in range(STEPS):
        owns[s][RB] = zero_block

    @pl.when(lat == 0)
    def _():
        for s in range(STEPS):
            rims[s][0][...] = jnp.zeros((HB, 2 * NT, BLOCK), BF16)

    @pl.when(lat == N_LAT - 1)
    def _():
        for s in range(STEPS):
            rims[s][1][...] = jnp.zeros((HB, 2 * NT, BLOCK), BF16)

    loads[0].wait()
    loads[1].wait()
    loads[2].wait()
    for b in range(RB):
        own_0[b] = jnp.concatenate([state0[:, cols(b)], tang0[:, cols(b)]], axis=0).astype(BF16)

    pl.semaphore_wait(barrier, len(LAT_PEERS) + len(LON_PEERS))
    send_rims(0)

    loads[9].wait()
    crow_copies = [
        pltpu.make_async_remote_copy(
            src_ref=crow_own,
            dst_ref=dst,
            send_sem=crow_send.at[i],
            recv_sem=crow_recv.at[i],
            device_id=at_lon((lon + step) % N_LON),
            device_id_type=MESH,
        )
        for i, (dst, step) in enumerate(((crow_low, 1), (crow_high, N_LON - 1)))
    ]
    for copy in crow_copies:
        copy.start()

    for i in range(3, 9):
        loads[i].wait()

    lane16 = lax.broadcasted_iota(jnp.int32, (NT, BLOCK), 1)
    row16 = lax.broadcasted_iota(jnp.int32, (NT, BLOCK), 0)
    spread = (lane16 % NT == row16).astype(F32)
    tiled = STEP_LENGTH * jnp.dot(
        coup[...], spread, precision=lax.Precision.HIGHEST, preferred_element_type=F32
    )
    tiled = jnp.concatenate([tiled, tiled], axis=0)
    lane32 = lax.broadcasted_iota(jnp.int32, (2 * NT, BLOCK), 1)
    row32 = lax.broadcasted_iota(jnp.int32, (2 * NT, BLOCK), 0)
    tiled_hi = tiled.astype(BF16).astype(F32)
    tiled_part = jnp.where(lane32 < 64, tiled_hi, tiled - tiled_hi)
    mixer = jnp.where((lane32 % 32) // NT == row32 // NT, tiled_part, 0.0).astype(BF16)

    local_region = region[...] - lat * (N_LON * REG_DEV)
    region_t = jnp.transpose(
        jnp.concatenate([local_region.astype(F32)] * (BLOCK // RB), axis=0), (1, 0)
    )

    def own_part(s):
        for b in range(RB):
            if s == 0:
                st, tg = state0[:, cols(b)], tang0[:, cols(b)]
            else:
                st, tg = stk[b, :NT], stk[b, NT:]
            squared = st * st
            inverse = 1.0 / (1.0 + squared)
            scaled = rate[b : b + 1, :] * inverse
            uptake = scaled * st
            slope = scaled * (1.0 - squared) * inverse * tg
            both = jnp.concatenate([uptake, slope], axis=0)
            both_hi = both.astype(BF16)
            both_lo = (both - both_hi.astype(F32)).astype(BF16)
            sources = jnp.dot(
                mixer,
                jnp.concatenate([both_hi, both_lo, both_hi, both_lo], axis=0),
                preferred_element_type=F32,
            )
            extra = lists[K - 1, b]
            extra = jnp.where(extra >= RB, RB, extra)
            gathered = jnp.concatenate([owns[s][b], owns[s][extra]], axis=1)
            weights = jnp.concatenate([coef[b, 0], coef[b, K - 1]], axis=0)
            moved = jnp.dot(gathered, weights, preferred_element_type=F32)
            acc[b] = jnp.concatenate([st, tg], axis=0) + (moved + sources)

    def rim_part(s, b):
        parts = [rims[s][d][lists[1 + d, b] % HB] for d in range(4)]
        gathered = jnp.concatenate(parts, axis=1)
        weights = coef[b, 1:5].reshape(4 * BLOCK, BLOCK)
        moved = jnp.dot(gathered, weights, preferred_element_type=F32)
        explicit = (acc[b] + moved).astype(BF16)
        return jnp.dot(explicit, impl[b], preferred_element_type=F32)

    own_part(0)
    await_rims(0)
    for b in range(RB):
        new = rim_part(0, b)
        stk[b] = new
        own_1[b] = new.astype(BF16)
    send_rims(1)
    own_part(1)

    lanes = lax.broadcasted_iota(jnp.int32, (BLOCK, BLOCK), 1).astype(F32)
    first = (lat * N_LON + lon - 1) * REG_DEV
    slot = (region[...] - first) & (N_LON * REG_DEV - 1)
    rows = lax.broadcasted_iota(jnp.int32, (32, BLOCK), 0)
    for b in range(RB):
        onehot_t[b] = jnp.where(region_t[:, b : b + 1] == lanes, 1.0, 0.0).astype(BF16)
        onehot[:, cols(b)] = jnp.where(rows == slot[b : b + 1, :], 1.0, 0.0).astype(BF16)

    await_rims(1)
    partial = jnp.zeros((2 * NT, BLOCK), F32)
    for b in range(RB):
        new = rim_part(1, b)
        state_out[:, cols(b)] = new[:NT]
        residual = new[NT:] - tang0[:, cols(b)]
        precond_out[:, cols(b)] = residual
        high = residual.astype(BF16)
        low = (residual - high.astype(F32)).astype(BF16)
        partial += jnp.dot(
            jnp.concatenate([high, low], axis=0), onehot_t[b], preferred_element_type=F32
        )
    partial = partial[:NT] + partial[NT:]
    tile_lon[...] = partial.astype(BF16)

    def peer_copies(src, buf, peers, peer, send_sem, recv_sem):
        return [
            pltpu.make_async_remote_copy(
                src_ref=src,
                dst_ref=buf.at[i],
                send_sem=send_sem.at[i],
                recv_sem=recv_sem.at[i],
                device_id=peer(*p),
                device_id_type=MESH,
            )
            for i, p in enumerate(peers)
        ]

    lon_copies = peer_copies(tile_lon, lon_buf, LON_PEERS, lon_peer, lon_send, lon_recv)
    for copy in lon_copies:
        copy.start()

    for copy in crow_copies:
        copy.wait_recv()
    zero_rows = jnp.zeros((REG_DEV, BLOCK), F32)
    for dz in range(NZ):
        parts = []
        for dx in range(NX):
            other = ((z + NZ - dz) % NZ) * NX + (x + NX - dx) % NX
            at = pl.ds(pl.multiple_of(other * BLOCK, BLOCK), BLOCK)
            parts += [crow_low[:, at], crow_own[:, at], crow_high[:, at], zero_rows]
        coarse_w[dz] = jnp.transpose(jnp.concatenate(parts, axis=0), (1, 0)).astype(BF16)

    totals = partial.astype(BF16).astype(F32)
    for i, copy in enumerate(lon_copies):
        copy.wait_recv()
        totals += lon_buf[i].astype(F32)
    tile_lat[...] = totals.astype(BF16)

    lat_copies = peer_copies(tile_lat, lat_buf, LAT_PEERS, lat_peer, lat_send, lat_recv)
    for copy in lat_copies:
        copy.start()
    for copy in crow_copies + lon_copies:
        copy.wait_send()
    for s in range(STEPS):
        await_rim_sends(s)
    for copy in lat_copies:
        copy.wait_recv()

    values = jnp.zeros((NX * NT, BLOCK), F32)
    for dz in range(NZ):
        tiles = [
            tile_lat[...] if (dz, dx) == (0, 0) else lat_buf[LAT_PEERS.index((dz, dx))]
            for dx in range(NX)
        ]
        values += jnp.dot(
            jnp.concatenate(tiles, axis=0), coarse_w[dz], preferred_element_type=F32
        )
    own_values = values[:NT]
    for dx in range(1, NX):
        own_values += pltpu.roll(values[dx * NT : (dx + 1) * NT], BLOCK - 32 * dx, 1)
    own_values = own_values[:, :32]
    high = own_values.astype(BF16)
    low = (own_values - high.astype(F32)).astype(BF16)
    both = jnp.concatenate([high, low], axis=0)
    for b in range(RB):
        spread_b = jnp.dot(both, onehot[:, cols(b)], preferred_element_type=F32)
        precond_out[:, cols(b)] += spread_b[:NT] + spread_b[NT:]
    for copy in lat_copies:
        copy.wait_send()


def local(
    state_init,
    tangent_init,
    coef_blocks,
    column_lists,
    send_lists,
    implicit_blocks,
    uptake_rate,
    coupling,
    region_map,
    coarse_inverse,
):
    rows = RB * BLOCK
    any_spec = pl.BlockSpec(memory_space=pl.ANY)
    vmem_spec = pl.BlockSpec(memory_space=pltpu.VMEM)
    rim = pltpu.VMEM((HB, 2 * NT, BLOCK), BF16)
    return pl.pallas_call(
        kernel,
        name="tracer_step",
        out_shape=(
            jax.ShapeDtypeStruct((NT, rows), F32),
            jax.ShapeDtypeStruct((NT, rows), F32),
        ),
        in_specs=[any_spec] * 10,
        out_specs=(vmem_spec, vmem_spec),
        scratch_shapes=[
            pltpu.VMEM((NT, rows), F32),
            pltpu.VMEM((NT, rows), F32),
            pltpu.VMEM((RB, K, BLOCK, BLOCK), BF16),
            pltpu.VMEM((RB, BLOCK, BLOCK), BF16),
            pltpu.VMEM((RB, BLOCK), F32),
            pltpu.VMEM((NT, NT), F32),
            pltpu.VMEM((RB, BLOCK), jnp.int32),
            pltpu.VMEM((REG_DEV, N_LAT * BLOCK), F32),
            pltpu.VMEM((REG_DEV, N_LAT * BLOCK), F32),
            pltpu.VMEM((REG_DEV, N_LAT * BLOCK), F32),
            pltpu.SMEM((K, RB), jnp.int32),
            pltpu.SMEM((1, HB, 4), jnp.int32),
            pltpu.VMEM((RB + 1, 2 * NT, BLOCK), BF16),
            pltpu.VMEM((RB + 1, 2 * NT, BLOCK), BF16),
            rim,
            rim,
            rim,
            rim,
            rim,
            rim,
            rim,
            rim,
            pltpu.VMEM((STEPS, 4, HB, 2 * NT, BLOCK), BF16),
            pltpu.VMEM((RB, 2 * NT, BLOCK), F32),
            pltpu.VMEM((RB, 2 * NT, BLOCK), F32),
            pltpu.VMEM((RB, BLOCK, BLOCK), BF16),
            pltpu.VMEM((32, rows), BF16),
            pltpu.VMEM((NZ, BLOCK, BLOCK), BF16),
            pltpu.VMEM((NT, BLOCK), BF16),
            pltpu.VMEM((len(LON_PEERS), NT, BLOCK), BF16),
            pltpu.VMEM((NT, BLOCK), BF16),
            pltpu.VMEM((len(LAT_PEERS), NT, BLOCK), BF16),
            pltpu.SemaphoreType.DMA((10,)),
            pltpu.SemaphoreType.DMA((STEPS, 4)),
            pltpu.SemaphoreType.DMA((STEPS, 4)),
            pltpu.SemaphoreType.DMA((2,)),
            pltpu.SemaphoreType.DMA((2,)),
            pltpu.SemaphoreType.DMA((len(LON_PEERS),)),
            pltpu.SemaphoreType.DMA((len(LON_PEERS),)),
            pltpu.SemaphoreType.DMA((len(LAT_PEERS),)),
            pltpu.SemaphoreType.DMA((len(LAT_PEERS),)),
        ],
        compiler_params=pltpu.CompilerParams(collective_id=0, has_side_effects=True),
    )(
        state_init,
        tangent_init,
        coef_blocks,
        column_lists.T,
        send_lists.transpose(0, 2, 1),
        implicit_blocks,
        uptake_rate.reshape(RB, BLOCK),
        coupling,
        region_map.reshape(RB, BLOCK),
        coarse_inverse,
    )


def solution(mesh):
    torus = Mesh(mesh.devices.reshape(NZ, NX, NY, NCORE), AXES)
    placed = (
        P(None, AXES),
        P(None, AXES),
        P(AXES, None, None, None),
        P(AXES, None),
        P(AXES, None, None),
        P(AXES, None, None),
        P(AXES),
        P(),
        P(AXES),
        P(AXES, None),
    )
    return jax.shard_map(
        local,
        mesh=torus,
        in_specs=placed,
        out_specs=(P(None, AXES), P(None, AXES)),
        check_vma=False,
    )
```

```python
import jax
import jax.numpy as jnp
from jax import lax
from jax.experimental import pallas as pl
from jax.experimental.pallas import tpu as pltpu
from jax.sharding import Mesh
from jax.sharding import PartitionSpec as P

NT = 16
STEPS = 2
REG_DEV = 8
RB = 16
K = 6
HB = 2
BLOCK = 128
STEP_LENGTH = 0.5
AXES = ("z", "x", "y", "c")
NZ, NX, NY, NCORE = 8, 4, 8, 2
N_LAT = NZ * NX
N_LON = NY * NCORE
MESH = pl.DeviceIdType.MESH
F32 = jnp.float32
BF16 = jnp.bfloat16


def ring_hops(d, n):
    return min(d, n - d)


LON_PEERS = sorted(
    ((dy, dc) for dy in range(NY) for dc in range(NCORE) if (dy, dc) != (0, 0)),
    key=lambda p: -ring_hops(p[0], NY),
)
LAT_PEERS = sorted(
    ((dz, dx) for dz in range(NZ) for dx in range(NX) if (dz, dx) != (0, 0)),
    key=lambda p: -(ring_hops(p[0], NZ) + ring_hops(p[1], NX)),
)


def kernel(
    state_hbm,
    tangent_hbm,
    coef_hbm,
    lists_hbm,
    sends_hbm,
    implicit_hbm,
    rate_hbm,
    coupling_hbm,
    region_hbm,
    coarse_hbm,
    state_out,
    precond_out,
    state0,
    tang0,
    coef,
    impl,
    rate,
    coup,
    region,
    crow_own,
    crow_low,
    crow_high,
    lists,
    sends,
    own_0,
    own_1,
    rims_0,
    rims_1,
    rims_2,
    rims_3,
    rims_4,
    rims_5,
    rims_6,
    rims_7,
    picks,
    acc,
    explicit,
    split,
    stk,
    onehot_t,
    onehot,
    coarse_w,
    tile_lon,
    lon_buf,
    tile_lat,
    lat_buf,
    load_sem,
    rim_send,
    rim_recv,
    crow_send,
    crow_recv,
    lon_send,
    lon_recv,
    lat_send,
    lat_recv,
    known,
):
    z, x = lax.axis_index("z"), lax.axis_index("x")
    y, c = lax.axis_index("y"), lax.axis_index("c")
    lat = z * NX + x
    lon = y * NCORE + c
    owns = (own_0, own_1)
    rims = ((rims_0, rims_1, rims_2, rims_3), (rims_4, rims_5, rims_6, rims_7))

    def at_lat(v):
        return (v // NX, v % NX, y, c)

    def at_lon(v):
        return (z, x, v // NCORE, v % NCORE)

    def lon_peer(dy, dc):
        return (z, x, (y + dy) % NY, (c + dc) % NCORE)

    def lat_peer(dz, dx):
        return ((z + dz) % NZ, (x + dx) % NX, y, c)

    pairs = (
        (sends_hbm, sends),
        (state_hbm, state0),
        (tangent_hbm, tang0),
        (lists_hbm, lists),
        (rate_hbm, rate),
        (coupling_hbm, coup),
        (region_hbm, region),
        (coef_hbm, coef),
        (implicit_hbm, impl),
        (coarse_hbm, crow_own),
    )
    loads = [pltpu.make_async_copy(a, b, load_sem.at[i]) for i, (a, b) in enumerate(pairs)]
    for load in loads:
        load.start()

    def signal(sem, peer):
        pl.semaphore_signal(sem, inc=1, device_id=peer, device_id_type=MESH)

    def lon_at(step):
        return at_lon((lon + step + N_LON) % N_LON)

    def z_at(step):
        return lat_peer(step + NZ, 0)

    def x_at(step):
        return lat_peer(0, step + NX)

    barrier = pltpu.get_barrier_semaphore()
    for step in (1, -1):
        signal(barrier, at_lat((lat + step + N_LAT) % N_LAT))
        signal(barrier, lon_at(step))
        signal(barrier, z_at(step))
        signal(barrier, x_at(step))

    def tell(stage):
        if stage == 0:
            told = [(0, lon_at(1)), (0, lon_at(-1)), (1, z_at(1)), (1, z_at(-1))]
            told += [(2, x_at(1)), (2, x_at(-1))]
        elif stage == 1:
            told = [(3, lon_at(2)), (3, lon_at(-2)), (4, z_at(2)), (4, z_at(-2))]
        else:
            told = [(5, lon_at(4)), (5, lon_at(-4))] + [(6, x_at(i)) for i in range(1, NX)]
        for i, peer in told:
            signal(known.at[i], peer)

    def hear(stage):
        for i, count in (((0, 2), (1, 2), (2, 2)), ((3, 2), (4, 2)), ((5, 2), (6, NX - 1)))[stage]:
            pl.semaphore_wait(known.at[i], count)

    def cols(b):
        return slice(b * BLOCK, (b + 1) * BLOCK)

    def rim_copies(s):
        below, above = (lat + N_LAT - 1) % N_LAT, (lat + 1) % N_LAT
        west, east = (lon + N_LON - 1) % N_LON, (lon + 1) % N_LON
        targets = (at_lat(above), at_lat(below), at_lon(east), at_lon(west))
        return [
            pltpu.make_async_remote_copy(
                src_ref=picks.at[s, d],
                dst_ref=rims[s][d],
                send_sem=rim_send.at[s, d],
                recv_sem=rim_recv.at[s, d],
                device_id=targets[d],
                device_id_type=MESH,
            )
            for d in range(4)
        ]

    def send_rims(s):
        for d in range(4):
            for h in range(HB):
                picks[s, d, h] = owns[s][sends[0, h, d]]
        copies = rim_copies(s)

        @pl.when(lat < N_LAT - 1)
        def _():
            copies[0].start()

        @pl.when(lat > 0)
        def _():
            copies[1].start()

        copies[2].start()
        copies[3].start()

    def await_rims(s):
        copies = rim_copies(s)

        @pl.when(lat > 0)
        def _():
            copies[0].wait_recv()

        @pl.when(lat < N_LAT - 1)
        def _():
            copies[1].wait_recv()

        copies[2].wait_recv()
        copies[3].wait_recv()

    def await_rim_sends(s):
        copies = rim_copies(s)

        @pl.when(lat < N_LAT - 1)
        def _():
            copies[0].wait_send()

        @pl.when(lat > 0)
        def _():
            copies[1].wait_send()

        copies[2].wait_send()
        copies[3].wait_send()

    zero_block = jnp.zeros((2 * NT, BLOCK), BF16)
    for s in range(STEPS):
        owns[s][RB] = zero_block

    @pl.when(lat == 0)
    def _():
        for s in range(STEPS):
            rims[s][0][...] = jnp.zeros((HB, 2 * NT, BLOCK), BF16)

    @pl.when(lat == N_LAT - 1)
    def _():
        for s in range(STEPS):
            rims[s][1][...] = jnp.zeros((HB, 2 * NT, BLOCK), BF16)

    loads[0].wait()
    loads[1].wait()
    loads[2].wait()
    for b in range(RB):
        own_0[b] = jnp.concatenate([state0[:, cols(b)], tang0[:, cols(b)]], axis=0).astype(BF16)

    pl.semaphore_wait(barrier, 8)
    send_rims(0)
    tell(0)

    crow_copies = [
        pltpu.make_async_remote_copy(
            src_ref=crow_own,
            dst_ref=dst,
            send_sem=crow_send.at[i],
            recv_sem=crow_recv.at[i],
            device_id=at_lon((lon + step) % N_LON),
            device_id_type=MESH,
        )
        for i, (dst, step) in enumerate(((crow_low, 1), (crow_high, N_LON - 1)))
    ]

    for i in range(3, 9):
        loads[i].wait()

    lane16 = lax.broadcasted_iota(jnp.int32, (NT, BLOCK), 1)
    row16 = lax.broadcasted_iota(jnp.int32, (NT, BLOCK), 0)
    spread = (lane16 % NT == row16).astype(F32)
    tiled = STEP_LENGTH * jnp.dot(
        coup[...], spread, precision=lax.Precision.HIGHEST, preferred_element_type=F32
    )
    tiled = jnp.concatenate([tiled, tiled], axis=0)
    lane32 = lax.broadcasted_iota(jnp.int32, (2 * NT, BLOCK), 1)
    row32 = lax.broadcasted_iota(jnp.int32, (2 * NT, BLOCK), 0)
    tiled_hi = tiled.astype(BF16).astype(F32)
    tiled_part = jnp.where(lane32 < 64, tiled_hi, tiled - tiled_hi)
    mixer = jnp.where((lane32 % 32) // NT == row32 // NT, tiled_part, 0.0).astype(BF16)

    local_region = region[...] - lat * (N_LON * REG_DEV)
    region_t = jnp.transpose(
        jnp.concatenate([local_region.astype(F32)] * (BLOCK // RB), axis=0), (1, 0)
    )

    def own_part(s):
        for b in range(RB):
            if s == 0:
                st, tg = state0[:, cols(b)], tang0[:, cols(b)]
            else:
                st, tg = stk[b, :NT], stk[b, NT:]
            squared = st * st
            inverse = 1.0 / (1.0 + squared)
            scaled = rate[b : b + 1, :] * inverse
            uptake = scaled * st
            slope = scaled * (1.0 - squared) * inverse * tg
            both = jnp.concatenate([uptake, slope], axis=0)
            both_hi = both.astype(BF16)
            both_lo = (both - both_hi.astype(F32)).astype(BF16)
            sources = jnp.dot(
                mixer,
                jnp.concatenate([both_hi, both_lo, both_hi, both_lo], axis=0),
                preferred_element_type=F32,
            )
            extra = lists[K - 1, b]
            extra = jnp.where(extra >= RB, RB, extra)
            gathered = jnp.concatenate([owns[s][b], owns[s][extra]], axis=1)
            weights = jnp.concatenate([coef[b, 0], coef[b, K - 1]], axis=0)
            moved = jnp.dot(gathered, weights, preferred_element_type=F32)
            acc[b] = jnp.concatenate([st, tg], axis=0) + (moved + sources)

    def rim_part(s):
        for b in range(RB):
            parts = [rims[s][d][lists[1 + d, b] % HB] for d in range(4)]
            gathered = jnp.concatenate(parts, axis=1)
            weights = coef[b, 1:5].reshape(4 * BLOCK, BLOCK)
            moved = jnp.dot(gathered, weights, preferred_element_type=F32)
            explicit[b] = (acc[b] + moved).astype(BF16)

    def implicit_part(b):
        return jnp.dot(explicit[b], impl[b], preferred_element_type=F32)

    own_part(0)
    loads[9].wait()
    for copy in crow_copies:
        copy.start()
    await_rims(0)
    hear(0)
    tell(1)
    rim_part(0)
    for b in range(RB):
        new = implicit_part(b)
        stk[b] = new
        own_1[b] = new.astype(BF16)
    send_rims(1)
    own_part(1)
    hear(1)
    tell(2)

    lanes = lax.broadcasted_iota(jnp.int32, (BLOCK, BLOCK), 1).astype(F32)
    first = (lat * N_LON + lon - 1) * REG_DEV
    slot = (region[...] - first) & (N_LON * REG_DEV - 1)
    rows = lax.broadcasted_iota(jnp.int32, (32, BLOCK), 0)
    for b in range(RB):
        onehot_t[b] = jnp.where(region_t[:, b : b + 1] == lanes, 1.0, 0.0).astype(BF16)
        onehot[:, cols(b)] = jnp.where(rows == slot[b : b + 1, :], 1.0, 0.0).astype(BF16)

    await_rims(1)
    rim_part(1)
    for b in range(RB):
        new = implicit_part(b)
        state_out[:, cols(b)] = new[:NT]
        residual = new[NT:] - tang0[:, cols(b)]
        precond_out[:, cols(b)] = residual
        high = residual.astype(BF16)
        low = (residual - high.astype(F32)).astype(BF16)
        split[b] = jnp.concatenate([high, low], axis=0)
    partial = jnp.zeros((2 * NT, BLOCK), F32)
    for b in range(0, RB, 2):
        partial += jnp.dot(
            jnp.concatenate([split[b], split[b + 1]], axis=1),
            onehot_t[b : b + 2].reshape(2 * BLOCK, BLOCK),
            preferred_element_type=F32,
        )
    partial = partial[:NT] + partial[NT:]
    tile_lon[...] = partial.astype(BF16)

    def peer_copies(src, buf, peers, peer, send_sem, recv_sem):
        return [
            pltpu.make_async_remote_copy(
                src_ref=src,
                dst_ref=buf.at[i],
                send_sem=send_sem.at[i],
                recv_sem=recv_sem.at[i],
                device_id=peer(*p),
                device_id_type=MESH,
            )
            for i, p in enumerate(peers)
        ]

    hear(2)
    lon_copies = peer_copies(tile_lon, lon_buf, LON_PEERS, lon_peer, lon_send, lon_recv)
    for copy in lon_copies:
        copy.start()

    for copy in crow_copies:
        copy.wait_recv()
    zero_rows = jnp.zeros((REG_DEV, BLOCK), F32)
    for dz in range(NZ):
        parts = []
        for dx in range(NX):
            other = ((z + NZ - dz) % NZ) * NX + (x + NX - dx) % NX
            at = pl.ds(pl.multiple_of(other * BLOCK, BLOCK), BLOCK)
            parts += [crow_low[:, at], crow_own[:, at], crow_high[:, at], zero_rows]
        coarse_w[dz] = jnp.transpose(jnp.concatenate(parts, axis=0), (1, 0)).astype(BF16)

    totals = partial.astype(BF16).astype(F32)
    for i, copy in enumerate(lon_copies):
        copy.wait_recv()
        totals += lon_buf[i].astype(F32)
    tile_lat[...] = totals.astype(BF16)

    lat_copies = peer_copies(tile_lat, lat_buf, LAT_PEERS, lat_peer, lat_send, lat_recv)
    for copy in lat_copies:
        copy.start()
    for copy in crow_copies + lon_copies:
        copy.wait_send()
    for s in range(STEPS):
        await_rim_sends(s)
    for copy in lat_copies:
        copy.wait_recv()

    values = jnp.zeros((NX * NT, BLOCK), F32)
    for dz in range(NZ):
        tiles = [
            tile_lat[...] if (dz, dx) == (0, 0) else lat_buf[LAT_PEERS.index((dz, dx))]
            for dx in range(NX)
        ]
        values += jnp.dot(
            jnp.concatenate(tiles, axis=0), coarse_w[dz], preferred_element_type=F32
        )
    own_values = values[:NT]
    for dx in range(1, NX):
        own_values += pltpu.roll(values[dx * NT : (dx + 1) * NT], BLOCK - 32 * dx, 1)
    own_values = own_values[:, :32]
    high = own_values.astype(BF16)
    low = (own_values - high.astype(F32)).astype(BF16)
    both = jnp.concatenate([high, low], axis=0)
    for b in range(RB):
        spread_b = jnp.dot(both, onehot[:, cols(b)], preferred_element_type=F32)
        precond_out[:, cols(b)] += spread_b[:NT] + spread_b[NT:]
    for copy in lat_copies:
        copy.wait_send()


def write_kernel(state_ref, precond_ref, state_out, precond_out, sem):
    copies = [
        pltpu.make_async_copy(state_ref, state_out, sem.at[0]),
        pltpu.make_async_copy(precond_ref, precond_out, sem.at[1]),
    ]
    for copy in copies:
        copy.start()
    for copy in copies:
        copy.wait()


def local(
    state_init,
    tangent_init,
    coef_blocks,
    column_lists,
    send_lists,
    implicit_blocks,
    uptake_rate,
    coupling,
    region_map,
    coarse_inverse,
):
    rows = RB * BLOCK
    hbm_spec = pl.BlockSpec(memory_space=pltpu.HBM)
    vmem_spec = pl.BlockSpec(memory_space=pltpu.VMEM)
    rim = pltpu.VMEM((HB, 2 * NT, BLOCK), BF16)
    outs = (
        jax.ShapeDtypeStruct((NT, rows), F32),
        jax.ShapeDtypeStruct((NT, rows), F32),
    )
    results = pl.pallas_call(
        kernel,
        name="tracer_step",
        out_shape=outs,
        in_specs=[hbm_spec] * 10,
        out_specs=(vmem_spec, vmem_spec),
        scratch_shapes=[
            pltpu.VMEM((NT, rows), F32),
            pltpu.VMEM((NT, rows), F32),
            pltpu.VMEM((RB, K, BLOCK, BLOCK), BF16),
            pltpu.VMEM((RB, BLOCK, BLOCK), BF16),
            pltpu.VMEM((RB, BLOCK), F32),
            pltpu.VMEM((NT, NT), F32),
            pltpu.VMEM((RB, BLOCK), jnp.int32),
            pltpu.VMEM((REG_DEV, N_LAT * BLOCK), F32),
            pltpu.VMEM((REG_DEV, N_LAT * BLOCK), F32),
            pltpu.VMEM((REG_DEV, N_LAT * BLOCK), F32),
            pltpu.SMEM((K, RB), jnp.int32),
            pltpu.SMEM((1, HB, 4), jnp.int32),
            pltpu.VMEM((RB + 1, 2 * NT, BLOCK), BF16),
            pltpu.VMEM((RB + 1, 2 * NT, BLOCK), BF16),
            rim,
            rim,
            rim,
            rim,
            rim,
            rim,
            rim,
            rim,
            pltpu.VMEM((STEPS, 4, HB, 2 * NT, BLOCK), BF16),
            pltpu.VMEM((RB, 2 * NT, BLOCK), F32),
            pltpu.VMEM((RB, 2 * NT, BLOCK), BF16),
            pltpu.VMEM((RB, 2 * NT, BLOCK), BF16),
            pltpu.VMEM((RB, 2 * NT, BLOCK), F32),
            pltpu.VMEM((RB, BLOCK, BLOCK), BF16),
            pltpu.VMEM((32, rows), BF16),
            pltpu.VMEM((NZ, BLOCK, BLOCK), BF16),
            pltpu.VMEM((NT, BLOCK), BF16),
            pltpu.VMEM((len(LON_PEERS), NT, BLOCK), BF16),
            pltpu.VMEM((NT, BLOCK), BF16),
            pltpu.VMEM((len(LAT_PEERS), NT, BLOCK), BF16),
            pltpu.SemaphoreType.DMA((10,)),
            pltpu.SemaphoreType.DMA((STEPS, 4)),
            pltpu.SemaphoreType.DMA((STEPS, 4)),
            pltpu.SemaphoreType.DMA((2,)),
            pltpu.SemaphoreType.DMA((2,)),
            pltpu.SemaphoreType.DMA((len(LON_PEERS),)),
            pltpu.SemaphoreType.DMA((len(LON_PEERS),)),
            pltpu.SemaphoreType.DMA((len(LAT_PEERS),)),
            pltpu.SemaphoreType.DMA((len(LAT_PEERS),)),
            pltpu.SemaphoreType.REGULAR((7,)),
        ],
        compiler_params=pltpu.CompilerParams(
            collective_id=0, has_side_effects=True, vmem_limit_bytes=24 * 2**20
        ),
    )(
        *(
            pltpu.with_memory_space_constraint(value, pltpu.HBM)
            for value in (
                state_init,
                tangent_init,
                coef_blocks,
                column_lists.T,
                send_lists.transpose(0, 2, 1),
                implicit_blocks,
                uptake_rate.reshape(RB, BLOCK),
                coupling,
                region_map.reshape(RB, BLOCK),
                coarse_inverse,
            )
        )
    )
    return pl.pallas_call(
        write_kernel,
        name="write_out",
        out_shape=outs,
        in_specs=[vmem_spec, vmem_spec],
        out_specs=(hbm_spec, hbm_spec),
        scratch_shapes=[pltpu.SemaphoreType.DMA((2,))],
        compiler_params=pltpu.CompilerParams(vmem_limit_bytes=4 * 2**20),
    )(*results)


def solution(mesh):
    torus = Mesh(mesh.devices.reshape(NZ, NX, NY, NCORE), AXES)
    placed = (
        P(None, AXES),
        P(None, AXES),
        P(AXES, None, None, None),
        P(AXES, None),
        P(AXES, None, None),
        P(AXES, None, None),
        P(AXES),
        P(),
        P(AXES),
        P(AXES, None),
    )
    return jax.shard_map(
        local,
        mesh=torus,
        in_specs=placed,
        out_specs=(P(None, AXES), P(None, AXES)),
        check_vma=False,
    )
```

```python
import jax
import jax.numpy as jnp
from jax import lax
from jax.experimental import pallas as pl
from jax.experimental.pallas import tpu as pltpu
from jax.sharding import Mesh
from jax.sharding import PartitionSpec as P

NT = 16
STEPS = 2
REG_DEV = 8
RB = 16
K = 6
HB = 2
BLOCK = 128
STEP_LENGTH = 0.5
AXES = ("z", "x", "y", "c")
NZ, NX, NY, NCORE = 8, 4, 8, 2
N_LAT = NZ * NX
N_LON = NY * NCORE
MESH = pl.DeviceIdType.MESH
F32 = jnp.float32
BF16 = jnp.bfloat16


def ring_hops(d, n):
    return min(d, n - d)


LON_PEERS = sorted(
    ((dy, dc) for dy in range(NY) for dc in range(NCORE) if (dy, dc) != (0, 0)),
    key=lambda p: -ring_hops(p[0], NY),
)

def kernel(
    state_hbm,
    tangent_hbm,
    coef_hbm,
    lists_hbm,
    sends_hbm,
    implicit_hbm,
    rate_hbm,
    coupling_hbm,
    region_hbm,
    coarse_hbm,
    state_out,
    precond_out,
    state0,
    tang0,
    coef,
    impl,
    rate,
    coup,
    region,
    crow_own,
    crow_side,
    lists,
    sends,
    own_0,
    own_1,
    rims_0,
    rims_1,
    rims_2,
    rims_3,
    rims_4,
    rims_5,
    rims_6,
    rims_7,
    picks,
    acc,
    explicit,
    split,
    stk,
    onehot_t,
    onehot,
    coarse_w,
    tile_lon,
    lon_buf,
    tile_lat,
    lat_buf,
    load_sem,
    rim_send,
    rim_recv,
    crow_send,
    crow_recv,
    lon_send,
    lon_recv,
    lat_send,
    lat_recv,
    known,
):
    z, x = lax.axis_index("z"), lax.axis_index("x")
    y, c = lax.axis_index("y"), lax.axis_index("c")
    lat = z * NX + x
    lon = y * NCORE + c
    owns = (own_0, own_1)
    rims = ((rims_0, rims_1, rims_2, rims_3), (rims_4, rims_5, rims_6, rims_7))

    def at_lat(v):
        return (v // NX, v % NX, y, c)

    def at_lon(v):
        return (z, x, v // NCORE, v % NCORE)

    def lon_peer(dy, dc):
        return (z, x, (y + dy) % NY, (c + dc) % NCORE)

    def torus_at(dz, dx):
        return ((z + dz) % NZ, (x + dx) % NX, y, c)

    pairs = (
        (sends_hbm, sends),
        (state_hbm, state0),
        (tangent_hbm, tang0),
        (lists_hbm, lists),
        (rate_hbm, rate),
        (coupling_hbm, coup),
        (region_hbm, region),
        (coef_hbm, coef),
        (implicit_hbm, impl),
        (coarse_hbm, crow_own),
    )
    loads = [pltpu.make_async_copy(a, b, load_sem.at[i]) for i, (a, b) in enumerate(pairs)]
    for load in loads:
        load.start()

    def signal(sem, peer):
        pl.semaphore_signal(sem, inc=1, device_id=peer, device_id_type=MESH)

    def lon_at(step):
        return at_lon((lon + step + N_LON) % N_LON)

    def z_at(step):
        return torus_at(step + NZ, 0)

    def x_at(step):
        return torus_at(0, step + NX)

    barrier = pltpu.get_barrier_semaphore()
    for step in (1, -1):
        signal(barrier, at_lat((lat + step + N_LAT) % N_LAT))
        signal(barrier, lon_at(step))
        signal(barrier, z_at(step))
        signal(barrier, x_at(step))

    def tell(stage):
        if stage == 0:
            told = [lon_at(1), lon_at(-1), z_at(1), z_at(-1), x_at(1), x_at(-1)]
        elif stage == 1:
            told = [lon_at(2), lon_at(-2), z_at(2), z_at(-2)]
        else:
            told = [lon_at(4), lon_at(-4)] + [x_at(i) for i in range(1, NX)]
        for peer in told:
            signal(known.at[stage], peer)

    def hear(stage):
        pl.semaphore_wait(known.at[stage], (6, 4, 5)[stage])

    def cols(b):
        return slice(b * BLOCK, (b + 1) * BLOCK)

    def rim_copies(s):
        below, above = (lat + N_LAT - 1) % N_LAT, (lat + 1) % N_LAT
        west, east = (lon + N_LON - 1) % N_LON, (lon + 1) % N_LON
        targets = (at_lat(above), at_lat(below), at_lon(east), at_lon(west))
        return [
            pltpu.make_async_remote_copy(
                src_ref=picks.at[s, d],
                dst_ref=rims[s][d],
                send_sem=rim_send.at[d],
                recv_sem=rim_recv.at[s, d],
                device_id=targets[d],
                device_id_type=MESH,
            )
            for d in range(4)
        ]

    def send_rims(s):
        for d in range(4):
            for h in range(HB):
                picks[s, d, h] = owns[s][sends[0, h, d]]
        copies = rim_copies(s)

        @pl.when(lat < N_LAT - 1)
        def _():
            copies[0].start()

        @pl.when(lat > 0)
        def _():
            copies[1].start()

        copies[2].start()
        copies[3].start()

    def await_rims(s):
        copies = rim_copies(s)

        @pl.when(lat > 0)
        def _():
            copies[0].wait_recv()

        @pl.when(lat < N_LAT - 1)
        def _():
            copies[1].wait_recv()

        copies[2].wait_recv()
        copies[3].wait_recv()

    def await_rim_sends(s):
        copies = rim_copies(s)

        @pl.when(lat < N_LAT - 1)
        def _():
            copies[0].wait_send()

        @pl.when(lat > 0)
        def _():
            copies[1].wait_send()

        copies[2].wait_send()
        copies[3].wait_send()

    zero_block = jnp.zeros((2 * NT, BLOCK), BF16)
    for s in range(STEPS):
        owns[s][RB] = zero_block

    @pl.when(lat == 0)
    def _():
        for s in range(STEPS):
            rims[s][0][...] = jnp.zeros((HB, 2 * NT, BLOCK), BF16)

    @pl.when(lat == N_LAT - 1)
    def _():
        for s in range(STEPS):
            rims[s][1][...] = jnp.zeros((HB, 2 * NT, BLOCK), BF16)

    loads[0].wait()
    loads[1].wait()
    loads[2].wait()
    for b in range(RB):
        own_0[b] = jnp.concatenate([state0[:, cols(b)], tang0[:, cols(b)]], axis=0).astype(BF16)

    pl.semaphore_wait(barrier, 8)
    send_rims(0)
    tell(0)

    crow_copies = [
        pltpu.make_async_remote_copy(
            src_ref=crow_own,
            dst_ref=crow_side.at[i],
            send_sem=crow_send,
            recv_sem=crow_recv,
            device_id=lon_at(step),
            device_id_type=MESH,
        )
        for i, step in enumerate((1, -1))
    ]

    def group(ref, send_sem, recv_sem):
        return pltpu.make_async_remote_copy(
            src_ref=ref,
            dst_ref=ref,
            send_sem=send_sem,
            recv_sem=recv_sem,
            device_id=lon_at(1),
            device_id_type=MESH,
        )

    crow_all = group(crow_side, crow_send, crow_recv)

    for i in range(3, 9):
        loads[i].wait()

    lane16 = lax.broadcasted_iota(jnp.int32, (NT, BLOCK), 1)
    row16 = lax.broadcasted_iota(jnp.int32, (NT, BLOCK), 0)
    spread = (lane16 % NT == row16).astype(F32)
    tiled = STEP_LENGTH * jnp.dot(
        coup[...], spread, precision=lax.Precision.HIGHEST, preferred_element_type=F32
    )
    tiled = jnp.concatenate([tiled, tiled], axis=0)
    lane32 = lax.broadcasted_iota(jnp.int32, (2 * NT, BLOCK), 1)
    row32 = lax.broadcasted_iota(jnp.int32, (2 * NT, BLOCK), 0)
    tiled_hi = tiled.astype(BF16).astype(F32)
    tiled_part = jnp.where(lane32 < 64, tiled_hi, tiled - tiled_hi)
    mixer = jnp.where((lane32 % 32) // NT == row32 // NT, tiled_part, 0.0).astype(BF16)

    local_region = region[...] - lat * (N_LON * REG_DEV)
    region_t = jnp.transpose(
        jnp.concatenate([local_region.astype(F32)] * (BLOCK // RB), axis=0), (1, 0)
    )

    def own_part(s):
        for b in range(RB):
            if s == 0:
                st, tg = state0[:, cols(b)], tang0[:, cols(b)]
            else:
                st, tg = stk[b, :NT], stk[b, NT:]
            squared = st * st
            inverse = 1.0 / (1.0 + squared)
            scaled = rate[b : b + 1, :] * inverse
            uptake = scaled * st
            slope = scaled * (1.0 - squared) * inverse * tg
            both = jnp.concatenate([uptake, slope], axis=0)
            both_hi = both.astype(BF16)
            both_lo = (both - both_hi.astype(F32)).astype(BF16)
            sources = jnp.dot(
                mixer,
                jnp.concatenate([both_hi, both_lo, both_hi, both_lo], axis=0),
                preferred_element_type=F32,
            )
            extra = lists[K - 1, b]
            extra = jnp.where(extra >= RB, RB, extra)
            gathered = jnp.concatenate([owns[s][b], owns[s][extra]], axis=1)
            weights = jnp.concatenate([coef[b, 0], coef[b, K - 1]], axis=0)
            moved = jnp.dot(gathered, weights, preferred_element_type=F32)
            acc[b] = jnp.concatenate([st, tg], axis=0) + (moved + sources)

    def rim_part(s):
        for b in range(RB):
            parts = [rims[s][d][lists[1 + d, b] % HB] for d in range(4)]
            gathered = jnp.concatenate(parts, axis=1)
            weights = coef[b, 1:5].reshape(4 * BLOCK, BLOCK)
            moved = jnp.dot(gathered, weights, preferred_element_type=F32)
            explicit[b] = (acc[b] + moved).astype(BF16)

    def implicit_part(b):
        return jnp.dot(explicit[b], impl[b], preferred_element_type=F32)

    own_part(0)
    loads[9].wait()
    for copy in crow_copies:
        copy.start()
    hear(0)
    tell(1)
    await_rims(0)
    rim_part(0)
    for b in range(RB):
        new = implicit_part(b)
        stk[b] = new
        own_1[b] = new.astype(BF16)
    await_rim_sends(0)
    send_rims(1)
    hear(1)
    tell(2)
    own_part(1)

    lanes = lax.broadcasted_iota(jnp.int32, (BLOCK, BLOCK), 1).astype(F32)
    first = (lat * N_LON + lon - 1) * REG_DEV
    slot = (region[...] - first) & (N_LON * REG_DEV - 1)
    rows = lax.broadcasted_iota(jnp.int32, (BLOCK, BLOCK), 0) % 32
    for b in range(RB):
        onehot_t[b] = jnp.where(region_t[:, b : b + 1] == lanes, 1.0, 0.0).astype(BF16)
        onehot[:, cols(b)] = jnp.where(rows == slot[b : b + 1, :], 1.0, 0.0).astype(BF16)

    await_rims(1)
    rim_part(1)
    for b in range(RB):
        new = implicit_part(b)
        state_out[:, cols(b)] = new[:NT]
        residual = new[NT:] - tang0[:, cols(b)]
        precond_out[:, cols(b)] = residual
        high = residual.astype(BF16)
        low = (residual - high.astype(F32)).astype(BF16)
        split[b] = jnp.concatenate([high, low], axis=0)
    partial = jnp.zeros((2 * NT, BLOCK), F32)
    for b in range(0, RB, 2):
        partial += jnp.dot(
            jnp.concatenate([split[b], split[b + 1]], axis=1),
            onehot_t[b : b + 2].reshape(2 * BLOCK, BLOCK),
            preferred_element_type=F32,
        )
    partial = partial[:NT] + partial[NT:]
    tile_lon[...] = partial.astype(BF16)

    hear(2)
    for i, p in enumerate(LON_PEERS):
        pltpu.make_async_remote_copy(
            src_ref=tile_lon,
            dst_ref=lon_buf.at[i],
            send_sem=lon_send,
            recv_sem=lon_recv,
            device_id=lon_peer(*p),
            device_id_type=MESH,
        ).start()

    crow_all.wait_recv()
    zero_rows = jnp.zeros((REG_DEV, BLOCK), F32)
    for k in range(NZ):
        parts = []
        for i in range(NX):
            at = cols(k * NX + i)
            parts += [crow_side[0, :, at], crow_own[:, at], crow_side[1, :, at], zero_rows]
        coarse_w[k] = jnp.transpose(jnp.concatenate(parts, axis=0), (1, 0)).astype(BF16)

    totals = partial.astype(BF16).astype(F32)
    lon_all = group(lon_buf, lon_send, lon_recv)
    lon_all.wait_recv()
    for i in range(len(LON_PEERS)):
        totals += lon_buf[i].astype(F32)
    tile_lat[...] = totals.astype(BF16)
    lat_buf[lat] = totals.astype(BF16)

    for i in range(N_LAT - 1):
        peer = jnp.where(lat <= i, i + 1, i)
        pltpu.make_async_remote_copy(
            src_ref=tile_lat,
            dst_ref=lat_buf.at[lat],
            send_sem=lat_send,
            recv_sem=lat_recv,
            device_id=at_lat(peer),
            device_id_type=MESH,
        ).start()
    crow_all.wait_send()
    lon_all.wait_send()
    await_rim_sends(1)
    lat_all = group(lat_buf.at[pl.ds(0, N_LAT - 1)], lat_send, lat_recv)
    lat_all.wait_recv()

    tiles = [lat_buf[NX * k : NX * (k + 1)].reshape(NX * NT, BLOCK) for k in range(NZ)]
    values = jnp.dot(
        jnp.concatenate(tiles, axis=1),
        coarse_w[...].reshape(NZ * BLOCK, BLOCK),
        preferred_element_type=F32,
    )
    own_values = jnp.where(lane16 // 32 == 0, values[:NT], 0.0)
    for i in range(1, NX):
        own_values += jnp.where(lane16 // 32 == i, values[i * NT : (i + 1) * NT], 0.0)
    high = own_values.astype(BF16)
    low = (own_values - high.astype(F32)).astype(BF16)
    spread_values = jnp.dot(
        jnp.concatenate([high, low], axis=0), onehot[...], preferred_element_type=F32
    )
    precond_out[...] += spread_values[:NT] + spread_values[NT:]
    lat_all.wait_send()


def write_kernel(state_ref, precond_ref, state_out, precond_out, sem):
    copies = [
        pltpu.make_async_copy(state_ref, state_out, sem.at[0]),
        pltpu.make_async_copy(precond_ref, precond_out, sem.at[1]),
    ]
    for copy in copies:
        copy.start()
    for copy in copies:
        copy.wait()


def local(
    state_init,
    tangent_init,
    coef_blocks,
    column_lists,
    send_lists,
    implicit_blocks,
    uptake_rate,
    coupling,
    region_map,
    coarse_inverse,
):
    rows = RB * BLOCK
    hbm_spec = pl.BlockSpec(memory_space=pltpu.HBM)
    vmem_spec = pl.BlockSpec(memory_space=pltpu.VMEM)
    rim = pltpu.VMEM((HB, 2 * NT, BLOCK), BF16)
    outs = (
        jax.ShapeDtypeStruct((NT, rows), F32),
        jax.ShapeDtypeStruct((NT, rows), F32),
    )
    results = pl.pallas_call(
        kernel,
        name="tracer_step",
        out_shape=outs,
        in_specs=[hbm_spec] * 10,
        out_specs=(vmem_spec, vmem_spec),
        scratch_shapes=[
            pltpu.VMEM((NT, rows), F32),
            pltpu.VMEM((NT, rows), F32),
            pltpu.VMEM((RB, K, BLOCK, BLOCK), BF16),
            pltpu.VMEM((RB, BLOCK, BLOCK), BF16),
            pltpu.VMEM((RB, BLOCK), F32),
            pltpu.VMEM((NT, NT), F32),
            pltpu.VMEM((RB, BLOCK), jnp.int32),
            pltpu.VMEM((REG_DEV, N_LAT * BLOCK), F32),
            pltpu.VMEM((2, REG_DEV, N_LAT * BLOCK), F32),
            pltpu.SMEM((K, RB), jnp.int32),
            pltpu.SMEM((1, HB, 4), jnp.int32),
            pltpu.VMEM((RB + 1, 2 * NT, BLOCK), BF16),
            pltpu.VMEM((RB + 1, 2 * NT, BLOCK), BF16),
            rim,
            rim,
            rim,
            rim,
            rim,
            rim,
            rim,
            rim,
            pltpu.VMEM((STEPS, 4, HB, 2 * NT, BLOCK), BF16),
            pltpu.VMEM((RB, 2 * NT, BLOCK), F32),
            pltpu.VMEM((RB, 2 * NT, BLOCK), BF16),
            pltpu.VMEM((RB, 2 * NT, BLOCK), BF16),
            pltpu.VMEM((RB, 2 * NT, BLOCK), F32),
            pltpu.VMEM((RB, BLOCK, BLOCK), BF16),
            pltpu.VMEM((BLOCK, rows), BF16),
            pltpu.VMEM((NZ, BLOCK, BLOCK), BF16),
            pltpu.VMEM((NT, BLOCK), BF16),
            pltpu.VMEM((len(LON_PEERS), NT, BLOCK), BF16),
            pltpu.VMEM((NT, BLOCK), BF16),
            pltpu.VMEM((N_LAT, NT, BLOCK), BF16),
            pltpu.SemaphoreType.DMA((10,)),
            pltpu.SemaphoreType.DMA((4,)),
            pltpu.SemaphoreType.DMA((STEPS, 4)),
            pltpu.SemaphoreType.DMA,
            pltpu.SemaphoreType.DMA,
            pltpu.SemaphoreType.DMA,
            pltpu.SemaphoreType.DMA,
            pltpu.SemaphoreType.DMA,
            pltpu.SemaphoreType.DMA,
            pltpu.SemaphoreType.REGULAR((3,)),
        ],
        compiler_params=pltpu.CompilerParams(
            collective_id=0, has_side_effects=True, vmem_limit_bytes=24 * 2**20
        ),
    )(
        *(
            pltpu.with_memory_space_constraint(value, pltpu.HBM)
            for value in (
                state_init,
                tangent_init,
                coef_blocks,
                column_lists.T,
                send_lists.transpose(0, 2, 1),
                implicit_blocks,
                uptake_rate.reshape(RB, BLOCK),
                coupling,
                region_map.reshape(RB, BLOCK),
                coarse_inverse,
            )
        )
    )
    return pl.pallas_call(
        write_kernel,
        name="write_out",
        out_shape=outs,
        in_specs=[vmem_spec, vmem_spec],
        out_specs=(hbm_spec, hbm_spec),
        scratch_shapes=[pltpu.SemaphoreType.DMA((2,))],
        compiler_params=pltpu.CompilerParams(vmem_limit_bytes=4 * 2**20),
    )(*results)


def solution(mesh):
    torus = Mesh(mesh.devices.reshape(NZ, NX, NY, NCORE), AXES)
    placed = (
        P(None, AXES),
        P(None, AXES),
        P(AXES, None, None, None),
        P(AXES, None),
        P(AXES, None, None),
        P(AXES, None, None),
        P(AXES),
        P(),
        P(AXES),
        P(AXES, None),
    )
    return jax.shard_map(
        local,
        mesh=torus,
        in_specs=placed,
        out_specs=(P(None, AXES), P(None, AXES)),
        check_vma=False,
    )
```

```python
import jax
import jax.numpy as jnp
from jax import lax
from jax.experimental import pallas as pl
from jax.experimental.pallas import tpu as pltpu
from jax.sharding import Mesh
from jax.sharding import PartitionSpec as P

NT = 16
STEPS = 2
REG_DEV = 8
RB = 16
K = 6
HB = 2
BLOCK = 128
STEP_LENGTH = 0.5
AXES = ("z", "x", "y", "c")
NZ, NX, NY, NCORE = 8, 4, 8, 2
N_LAT = NZ * NX
N_LON = NY * NCORE
MESH = pl.DeviceIdType.MESH
F32 = jnp.float32
BF16 = jnp.bfloat16


def ring_hops(d, n):
    return min(d, n - d)


LON_PEERS = sorted(
    ((dy, dc) for dy in range(NY) for dc in range(NCORE) if (dy, dc) != (0, 0)),
    key=lambda p: -ring_hops(p[0], NY),
)

def kernel(
    state_hbm,
    tangent_hbm,
    coef_hbm,
    lists_hbm,
    sends_hbm,
    implicit_hbm,
    rate_hbm,
    coupling_hbm,
    region_hbm,
    coarse_hbm,
    state_out,
    precond_out,
    state0,
    tang0,
    coef,
    impl,
    rate,
    coup,
    region,
    crow_own,
    crow_side,
    lists,
    sends,
    own_0,
    own_1,
    rims_0,
    rims_1,
    rims_2,
    rims_3,
    rims_4,
    rims_5,
    rims_6,
    rims_7,
    picks,
    acc,
    explicit,
    folded,
    rim_w,
    stk,
    onehot_t,
    onehot,
    coarse_w,
    tile_lon,
    lon_buf,
    tile_lat,
    lat_buf,
    load_sem,
    rim_send,
    rim_recv,
    crow_send,
    crow_recv,
    lon_send,
    lon_recv,
    lat_send,
    lat_recv,
    known,
):
    z, x = lax.axis_index("z"), lax.axis_index("x")
    y, c = lax.axis_index("y"), lax.axis_index("c")
    lat = z * NX + x
    lon = y * NCORE + c
    owns = (own_0, own_1)
    rims = ((rims_0, rims_1, rims_2, rims_3), (rims_4, rims_5, rims_6, rims_7))

    def at_lat(v):
        return (v // NX, v % NX, y, c)

    def at_lon(v):
        return (z, x, v // NCORE, v % NCORE)

    def lon_peer(dy, dc):
        return (z, x, (y + dy) % NY, (c + dc) % NCORE)

    def torus_at(dz, dx):
        return ((z + dz) % NZ, (x + dx) % NX, y, c)

    pairs = (
        (sends_hbm, sends),
        (state_hbm, state0),
        (tangent_hbm, tang0),
        (lists_hbm, lists),
        (rate_hbm, rate),
        (coupling_hbm, coup),
        (region_hbm, region),
        (coef_hbm, coef),
        (implicit_hbm, impl),
        (coarse_hbm, crow_own),
    )
    loads = [pltpu.make_async_copy(a, b, load_sem.at[i]) for i, (a, b) in enumerate(pairs)]
    for load in loads:
        load.start()

    def signal(sem, peer):
        pl.semaphore_signal(sem, inc=1, device_id=peer, device_id_type=MESH)

    def lon_at(step):
        return at_lon((lon + step + N_LON) % N_LON)

    def z_at(step):
        return torus_at(step + NZ, 0)

    def x_at(step):
        return torus_at(0, step + NX)

    barrier = pltpu.get_barrier_semaphore()
    for step in (1, -1):
        signal(barrier, at_lat((lat + step + N_LAT) % N_LAT))
        signal(barrier, lon_at(step))
        signal(barrier, z_at(step))
        signal(barrier, x_at(step))

    def tell(stage):
        if stage == 0:
            told = [lon_at(1), lon_at(-1), z_at(1), z_at(-1), x_at(1), x_at(-1)]
        elif stage == 1:
            told = [lon_at(2), lon_at(-2), z_at(2), z_at(-2)]
        else:
            told = [lon_at(4), lon_at(-4)] + [x_at(i) for i in range(1, NX)]
        for peer in told:
            signal(known.at[stage], peer)

    def hear(stage):
        pl.semaphore_wait(known.at[stage], (6, 4, 5)[stage])

    def cols(b):
        return slice(b * BLOCK, (b + 1) * BLOCK)

    def rim_copies(s):
        below, above = (lat + N_LAT - 1) % N_LAT, (lat + 1) % N_LAT
        west, east = (lon + N_LON - 1) % N_LON, (lon + 1) % N_LON
        targets = (at_lat(above), at_lat(below), at_lon(east), at_lon(west))
        return [
            pltpu.make_async_remote_copy(
                src_ref=picks.at[s, d],
                dst_ref=rims[s][d],
                send_sem=rim_send.at[d],
                recv_sem=rim_recv.at[s, d],
                device_id=targets[d],
                device_id_type=MESH,
            )
            for d in range(4)
        ]

    def send_rims(s):
        for d in range(4):
            for h in range(HB):
                picks[s, d, h] = owns[s][sends[0, h, d]]
        copies = rim_copies(s)

        @pl.when(lat < N_LAT - 1)
        def _():
            copies[0].start()

        @pl.when(lat > 0)
        def _():
            copies[1].start()

        copies[2].start()
        copies[3].start()

    def await_rims(s):
        copies = rim_copies(s)

        @pl.when(lat > 0)
        def _():
            copies[0].wait_recv()

        @pl.when(lat < N_LAT - 1)
        def _():
            copies[1].wait_recv()

        copies[2].wait_recv()
        copies[3].wait_recv()

    def await_rim_sends(s):
        copies = rim_copies(s)

        @pl.when(lat < N_LAT - 1)
        def _():
            copies[0].wait_send()

        @pl.when(lat > 0)
        def _():
            copies[1].wait_send()

        copies[2].wait_send()
        copies[3].wait_send()

    zero_block = jnp.zeros((2 * NT, BLOCK), BF16)
    for s in range(STEPS):
        owns[s][RB] = zero_block

    @pl.when(lat == 0)
    def _():
        for s in range(STEPS):
            rims[s][0][...] = jnp.zeros((HB, 2 * NT, BLOCK), BF16)

    @pl.when(lat == N_LAT - 1)
    def _():
        for s in range(STEPS):
            rims[s][1][...] = jnp.zeros((HB, 2 * NT, BLOCK), BF16)

    loads[0].wait()
    loads[1].wait()
    loads[2].wait()
    for b in range(RB):
        own_0[b] = jnp.concatenate([state0[:, cols(b)], tang0[:, cols(b)]], axis=0).astype(BF16)

    pl.semaphore_wait(barrier, 8)
    send_rims(0)
    tell(0)

    crow_copies = [
        pltpu.make_async_remote_copy(
            src_ref=crow_own,
            dst_ref=crow_side.at[i],
            send_sem=crow_send,
            recv_sem=crow_recv,
            device_id=lon_at(step),
            device_id_type=MESH,
        )
        for i, step in enumerate((1, -1))
    ]

    def group(ref, send_sem, recv_sem):
        return pltpu.make_async_remote_copy(
            src_ref=ref,
            dst_ref=ref,
            send_sem=send_sem,
            recv_sem=recv_sem,
            device_id=lon_at(1),
            device_id_type=MESH,
        )

    crow_all = group(crow_side, crow_send, crow_recv)

    for i in range(3, 9):
        loads[i].wait()

    lane16 = lax.broadcasted_iota(jnp.int32, (NT, BLOCK), 1)
    row16 = lax.broadcasted_iota(jnp.int32, (NT, BLOCK), 0)
    spread = (lane16 % NT == row16).astype(F32)
    tiled = STEP_LENGTH * jnp.dot(
        coup[...], spread, precision=lax.Precision.HIGHEST, preferred_element_type=F32
    )
    tiled = jnp.concatenate([tiled, tiled], axis=0)
    lane32 = lax.broadcasted_iota(jnp.int32, (2 * NT, BLOCK), 1)
    row32 = lax.broadcasted_iota(jnp.int32, (2 * NT, BLOCK), 0)
    tiled_hi = tiled.astype(BF16).astype(F32)
    tiled_part = jnp.where(lane32 < 64, tiled_hi, tiled - tiled_hi)
    mixer = jnp.where((lane32 % 32) // NT == row32 // NT, tiled_part, 0.0).astype(BF16)

    local_region = region[...] - lat * (N_LON * REG_DEV)
    region_t = jnp.transpose(
        jnp.concatenate([local_region.astype(F32)] * (BLOCK // RB), axis=0), (1, 0)
    )

    def own_part(s):
        for b in range(RB):
            if s == 0:
                st, tg = state0[:, cols(b)], tang0[:, cols(b)]
            else:
                st, tg = stk[b, :NT], stk[b, NT:]
            squared = st * st
            inverse = 1.0 / (1.0 + squared)
            scaled = rate[b : b + 1, :] * inverse
            uptake = scaled * st
            slope = scaled * (1.0 - squared) * inverse * tg
            both = jnp.concatenate([uptake, slope], axis=0)
            both_hi = both.astype(BF16)
            both_lo = (both - both_hi.astype(F32)).astype(BF16)
            sources = jnp.dot(
                mixer,
                jnp.concatenate([both_hi, both_lo, both_hi, both_lo], axis=0),
                preferred_element_type=F32,
            )
            extra = lists[K - 1, b]
            extra = jnp.where(extra >= RB, RB, extra)
            gathered = jnp.concatenate([owns[s][b], owns[s][extra]], axis=1)
            weights = jnp.concatenate([coef[b, 0], coef[b, K - 1]], axis=0)
            moved = jnp.dot(gathered, weights, preferred_element_type=F32)
            acc[b] = jnp.concatenate([st, tg], axis=0) + (moved + sources)

    def rim_part(s):
        for b in range(RB):
            parts = [rims[s][d][lists[1 + d, b] % HB] for d in range(4)]
            gathered = jnp.concatenate(parts, axis=1)
            weights = coef[b, 1:5].reshape(4 * BLOCK, BLOCK)
            moved = jnp.dot(gathered, weights, preferred_element_type=F32)
            explicit[b] = (acc[b] + moved).astype(BF16)

    def implicit_part(b):
        return jnp.dot(explicit[b], impl[b], preferred_element_type=F32)

    own_part(0)
    loads[9].wait()
    for copy in crow_copies:
        copy.start()
    hear(0)
    tell(1)
    await_rims(0)
    rim_part(0)
    for b in range(RB):
        new = implicit_part(b)
        stk[b] = new
        own_1[b] = new.astype(BF16)
    await_rim_sends(0)
    send_rims(1)
    hear(1)
    tell(2)
    own_part(1)

    lanes = lax.broadcasted_iota(jnp.int32, (BLOCK, BLOCK), 1).astype(F32)
    first = (lat * N_LON + lon - 1) * REG_DEV
    slot = (region[...] - first) & (N_LON * REG_DEV - 1)
    rows = lax.broadcasted_iota(jnp.int32, (BLOCK, BLOCK), 0) % 32
    for b in range(RB):
        onehot_t[b] = jnp.where(region_t[:, b : b + 1] == lanes, 1.0, 0.0).astype(BF16)
        onehot[:, cols(b)] = jnp.where(rows == slot[b : b + 1, :], 1.0, 0.0).astype(BF16)

    for b in range(RB):
        folded[b] = jnp.dot(impl[b], onehot_t[b], preferred_element_type=F32).astype(BF16)
    partial = jnp.zeros((NT, BLOCK), F32)
    for b in range(RB):
        partial += jnp.dot(
            jnp.concatenate([acc[b, NT:].astype(BF16), -own_0[b, NT:]], axis=1),
            jnp.concatenate([folded[b], onehot_t[b]], axis=0),
            preferred_element_type=F32,
        )
    for d in range(4):
        both = jnp.zeros((BLOCK, BLOCK), F32)
        second = jnp.zeros((BLOCK, BLOCK), F32)
        for b in range(RB):
            product = jnp.dot(coef[b, 1 + d], folded[b], preferred_element_type=F32)
            both += product
            second += product * (lists[1 + d, b] % HB).astype(F32)
        rim_w[HB * d] = (both - second).astype(BF16)
        rim_w[HB * d + 1] = second.astype(BF16)

    await_rims(1)
    tangents = [rims[1][d][h, NT:] for d in range(4) for h in range(HB)]
    partial += jnp.dot(
        jnp.concatenate(tangents, axis=1),
        rim_w[...].reshape(4 * HB * BLOCK, BLOCK),
        preferred_element_type=F32,
    )
    tile_lon[...] = partial.astype(BF16)

    hear(2)
    for i, p in enumerate(LON_PEERS):
        pltpu.make_async_remote_copy(
            src_ref=tile_lon,
            dst_ref=lon_buf.at[i],
            send_sem=lon_send,
            recv_sem=lon_recv,
            device_id=lon_peer(*p),
            device_id_type=MESH,
        ).start()

    rim_part(1)
    for b in range(RB):
        new = implicit_part(b)
        state_out[:, cols(b)] = new[:NT]
        precond_out[:, cols(b)] = new[NT:] - tang0[:, cols(b)]

    crow_all.wait_recv()
    zero_rows = jnp.zeros((REG_DEV, BLOCK), F32)
    for k in range(NZ):
        parts = []
        for i in range(NX):
            at = cols(k * NX + i)
            parts += [crow_side[0, :, at], crow_own[:, at], crow_side[1, :, at], zero_rows]
        coarse_w[k] = jnp.transpose(jnp.concatenate(parts, axis=0), (1, 0)).astype(BF16)

    totals = partial.astype(BF16).astype(F32)
    lon_all = group(lon_buf, lon_send, lon_recv)
    lon_all.wait_recv()
    for i in range(len(LON_PEERS)):
        totals += lon_buf[i].astype(F32)
    tile_lat[...] = totals.astype(BF16)
    lat_buf[lat] = totals.astype(BF16)

    for i in range(N_LAT - 1):
        peer = jnp.where(lat <= i, i + 1, i)
        pltpu.make_async_remote_copy(
            src_ref=tile_lat,
            dst_ref=lat_buf.at[lat],
            send_sem=lat_send,
            recv_sem=lat_recv,
            device_id=at_lat(peer),
            device_id_type=MESH,
        ).start()
    crow_all.wait_send()
    lon_all.wait_send()
    await_rim_sends(1)
    lat_all = group(lat_buf.at[pl.ds(0, N_LAT - 1)], lat_send, lat_recv)
    lat_all.wait_recv()

    tiles = [lat_buf[NX * k : NX * (k + 1)].reshape(NX * NT, BLOCK) for k in range(NZ)]
    values = jnp.dot(
        jnp.concatenate(tiles, axis=1),
        coarse_w[...].reshape(NZ * BLOCK, BLOCK),
        preferred_element_type=F32,
    )
    own_values = jnp.where(lane16 // 32 == 0, values[:NT], 0.0)
    for i in range(1, NX):
        own_values += jnp.where(lane16 // 32 == i, values[i * NT : (i + 1) * NT], 0.0)
    high = own_values.astype(BF16)
    low = (own_values - high.astype(F32)).astype(BF16)
    spread_values = jnp.dot(
        jnp.concatenate([high, low], axis=0), onehot[...], preferred_element_type=F32
    )
    precond_out[...] += spread_values[:NT] + spread_values[NT:]
    lat_all.wait_send()


def write_kernel(state_ref, precond_ref, state_out, precond_out, sem):
    copies = [
        pltpu.make_async_copy(state_ref, state_out, sem.at[0]),
        pltpu.make_async_copy(precond_ref, precond_out, sem.at[1]),
    ]
    for copy in copies:
        copy.start()
    for copy in copies:
        copy.wait()


def local(
    state_init,
    tangent_init,
    coef_blocks,
    column_lists,
    send_lists,
    implicit_blocks,
    uptake_rate,
    coupling,
    region_map,
    coarse_inverse,
):
    rows = RB * BLOCK
    hbm_spec = pl.BlockSpec(memory_space=pltpu.HBM)
    vmem_spec = pl.BlockSpec(memory_space=pltpu.VMEM)
    rim = pltpu.VMEM((HB, 2 * NT, BLOCK), BF16)
    outs = (
        jax.ShapeDtypeStruct((NT, rows), F32),
        jax.ShapeDtypeStruct((NT, rows), F32),
    )
    results = pl.pallas_call(
        kernel,
        name="tracer_step",
        out_shape=outs,
        in_specs=[hbm_spec] * 10,
        out_specs=(vmem_spec, vmem_spec),
        scratch_shapes=[
            pltpu.VMEM((NT, rows), F32),
            pltpu.VMEM((NT, rows), F32),
            pltpu.VMEM((RB, K, BLOCK, BLOCK), BF16),
            pltpu.VMEM((RB, BLOCK, BLOCK), BF16),
            pltpu.VMEM((RB, BLOCK), F32),
            pltpu.VMEM((NT, NT), F32),
            pltpu.VMEM((RB, BLOCK), jnp.int32),
            pltpu.VMEM((REG_DEV, N_LAT * BLOCK), F32),
            pltpu.VMEM((2, REG_DEV, N_LAT * BLOCK), F32),
            pltpu.SMEM((K, RB), jnp.int32),
            pltpu.SMEM((1, HB, 4), jnp.int32),
            pltpu.VMEM((RB + 1, 2 * NT, BLOCK), BF16),
            pltpu.VMEM((RB + 1, 2 * NT, BLOCK), BF16),
            rim,
            rim,
            rim,
            rim,
            rim,
            rim,
            rim,
            rim,
            pltpu.VMEM((STEPS, 4, HB, 2 * NT, BLOCK), BF16),
            pltpu.VMEM((RB, 2 * NT, BLOCK), F32),
            pltpu.VMEM((RB, 2 * NT, BLOCK), BF16),
            pltpu.VMEM((RB, BLOCK, BLOCK), BF16),
            pltpu.VMEM((4 * HB, BLOCK, BLOCK), BF16),
            pltpu.VMEM((RB, 2 * NT, BLOCK), F32),
            pltpu.VMEM((RB, BLOCK, BLOCK), BF16),
            pltpu.VMEM((BLOCK, rows), BF16),
            pltpu.VMEM((NZ, BLOCK, BLOCK), BF16),
            pltpu.VMEM((NT, BLOCK), BF16),
            pltpu.VMEM((len(LON_PEERS), NT, BLOCK), BF16),
            pltpu.VMEM((NT, BLOCK), BF16),
            pltpu.VMEM((N_LAT, NT, BLOCK), BF16),
            pltpu.SemaphoreType.DMA((10,)),
            pltpu.SemaphoreType.DMA((4,)),
            pltpu.SemaphoreType.DMA((STEPS, 4)),
            pltpu.SemaphoreType.DMA,
            pltpu.SemaphoreType.DMA,
            pltpu.SemaphoreType.DMA,
            pltpu.SemaphoreType.DMA,
            pltpu.SemaphoreType.DMA,
            pltpu.SemaphoreType.DMA,
            pltpu.SemaphoreType.REGULAR((3,)),
        ],
        compiler_params=pltpu.CompilerParams(
            collective_id=0, has_side_effects=True, vmem_limit_bytes=24 * 2**20
        ),
    )(
        *(
            pltpu.with_memory_space_constraint(value, pltpu.HBM)
            for value in (
                state_init,
                tangent_init,
                coef_blocks,
                column_lists.T,
                send_lists.transpose(0, 2, 1),
                implicit_blocks,
                uptake_rate.reshape(RB, BLOCK),
                coupling,
                region_map.reshape(RB, BLOCK),
                coarse_inverse,
            )
        )
    )
    return pl.pallas_call(
        write_kernel,
        name="write_out",
        out_shape=outs,
        in_specs=[vmem_spec, vmem_spec],
        out_specs=(hbm_spec, hbm_spec),
        scratch_shapes=[pltpu.SemaphoreType.DMA((2,))],
        compiler_params=pltpu.CompilerParams(vmem_limit_bytes=4 * 2**20),
    )(*results)


def solution(mesh):
    torus = Mesh(mesh.devices.reshape(NZ, NX, NY, NCORE), AXES)
    placed = (
        P(None, AXES),
        P(None, AXES),
        P(AXES, None, None, None),
        P(AXES, None),
        P(AXES, None, None),
        P(AXES, None, None),
        P(AXES),
        P(),
        P(AXES),
        P(AXES, None),
    )
    return jax.shard_map(
        local,
        mesh=torus,
        in_specs=placed,
        out_specs=(P(None, AXES), P(None, AXES)),
        check_vma=False,
    )
```

```python
import jax
import jax.numpy as jnp
from jax import lax
from jax.experimental import pallas as pl
from jax.experimental.pallas import tpu as pltpu
from jax.sharding import Mesh
from jax.sharding import PartitionSpec as P

NT = 16
STEPS = 2
REG_DEV = 8
RB = 16
K = 6
HB = 2
BLOCK = 128
STEP_LENGTH = 0.5
AXES = ("z", "x", "y", "c")
NZ, NX, NY, NCORE = 8, 4, 8, 2
N_LAT = NZ * NX
N_LON = NY * NCORE
MESH = pl.DeviceIdType.MESH
F32 = jnp.float32
BF16 = jnp.bfloat16


def ring_hops(d, n):
    return min(d, n - d)


LON_PEERS = sorted(
    ((dy, dc) for dy in range(NY) for dc in range(NCORE) if (dy, dc) != (0, 0)),
    key=lambda p: -ring_hops(p[0], NY),
)

def kernel(
    state_hbm,
    tangent_hbm,
    coef_hbm,
    lists_hbm,
    sends_hbm,
    implicit_hbm,
    rate_hbm,
    coupling_hbm,
    region_hbm,
    coarse_hbm,
    state_out,
    precond_out,
    state0,
    tang0,
    coef,
    impl,
    rate,
    coup,
    region,
    crow_own,
    crow_side,
    lists,
    sends,
    own_0,
    own_1,
    rims_0,
    rims_1,
    rims_2,
    rims_3,
    rims_4,
    rims_5,
    rims_6,
    rims_7,
    picks,
    acc,
    explicit,
    folded,
    rim_w,
    stk,
    onehot_t,
    onehot,
    coarse_w,
    tile_lon,
    lon_buf,
    tile_lat,
    lat_buf,
    load_sem,
    rim_send,
    rim_recv,
    crow_send,
    crow_recv,
    lon_send,
    lon_recv,
    lat_send,
    lat_recv,
    known,
):
    z, x = lax.axis_index("z"), lax.axis_index("x")
    y, c = lax.axis_index("y"), lax.axis_index("c")
    lat = z * NX + x
    lon = y * NCORE + c
    owns = (own_0, own_1)
    rims = ((rims_0, rims_1, rims_2, rims_3), (rims_4, rims_5, rims_6, rims_7))

    def at_lat(v):
        return (v // NX, v % NX, y, c)

    def at_lon(v):
        return (z, x, v // NCORE, v % NCORE)

    def lon_peer(dy, dc):
        return (z, x, (y + dy) % NY, (c + dc) % NCORE)

    def torus_at(dz, dx):
        return ((z + dz) % NZ, (x + dx) % NX, y, c)

    pairs = (
        (sends_hbm, sends),
        (state_hbm, state0),
        (tangent_hbm, tang0),
        (lists_hbm, lists),
        (rate_hbm, rate),
        (coupling_hbm, coup),
        (region_hbm, region),
        (coef_hbm, coef),
        (implicit_hbm, impl),
        (coarse_hbm, crow_own),
    )
    loads = [pltpu.make_async_copy(a, b, load_sem.at[i]) for i, (a, b) in enumerate(pairs)]
    for load in loads:
        load.start()

    def signal(sem, peer):
        pl.semaphore_signal(sem, inc=1, device_id=peer, device_id_type=MESH)

    def lon_at(step):
        return at_lon((lon + step + N_LON) % N_LON)

    def z_at(step):
        return torus_at(step + NZ, 0)

    def x_at(step):
        return torus_at(0, step + NX)

    def signal_z(sem, reach):
        @pl.when(z + reach < NZ)
        def _():
            signal(sem, z_at(reach))

        @pl.when(z >= reach)
        def _():
            signal(sem, z_at(-reach))

    def z_count(reach):
        return jnp.where(z + reach < NZ, 1, 0) + jnp.where(z >= reach, 1, 0)

    barrier = pltpu.get_barrier_semaphore()

    @pl.when(lat < N_LAT - 1)
    def _():
        signal(barrier, at_lat(lat + 1))

    @pl.when(lat > 0)
    def _():
        signal(barrier, at_lat(lat - 1))

    for step in (1, -1):
        signal(barrier, lon_at(step))
        signal(barrier, x_at(step))
    signal_z(barrier, 1)
    lat_count = jnp.where(lat < N_LAT - 1, 1, 0) + jnp.where(lat > 0, 1, 0)

    def tell(stage):
        sem = known.at[stage]
        if stage < 3:
            signal(sem, lon_at(2**stage))
            signal(sem, lon_at(-(2**stage)))
        if stage == 0:
            signal(sem, x_at(1))
            signal(sem, x_at(-1))
        if stage < 2:
            signal_z(sem, 2**stage)
        elif stage == 2:
            signal(sem, z_at(4))
        else:
            for i in range(1, NX):
                signal(sem, x_at(i))

    def hear(stage):
        counts = (4 + z_count(1), 2 + z_count(2), 3, NX - 1)
        pl.semaphore_wait(known.at[stage], counts[stage])

    def cols(b):
        return slice(b * BLOCK, (b + 1) * BLOCK)

    def rim_copies(s):
        below, above = (lat + N_LAT - 1) % N_LAT, (lat + 1) % N_LAT
        west, east = (lon + N_LON - 1) % N_LON, (lon + 1) % N_LON
        targets = (at_lat(above), at_lat(below), at_lon(east), at_lon(west))
        return [
            pltpu.make_async_remote_copy(
                src_ref=picks.at[s, d],
                dst_ref=rims[s][d],
                send_sem=rim_send.at[d],
                recv_sem=rim_recv.at[s, d],
                device_id=targets[d],
                device_id_type=MESH,
            )
            for d in range(4)
        ]

    def send_lat_rims(s):
        copies = rim_copies(s)

        @pl.when(lat < N_LAT - 1)
        def _():
            copies[0].start()

        @pl.when(lat > 0)
        def _():
            copies[1].start()

    def send_lon_rims(s):
        copies = rim_copies(s)
        copies[2].start()
        copies[3].start()

    def await_rims(s):
        copies = rim_copies(s)

        @pl.when(lat > 0)
        def _():
            copies[0].wait_recv()

        @pl.when(lat < N_LAT - 1)
        def _():
            copies[1].wait_recv()

        copies[2].wait_recv()
        copies[3].wait_recv()

    def await_rim_sends(s):
        copies = rim_copies(s)

        @pl.when(lat < N_LAT - 1)
        def _():
            copies[0].wait_send()

        @pl.when(lat > 0)
        def _():
            copies[1].wait_send()

        copies[2].wait_send()
        copies[3].wait_send()

    zero_block = jnp.zeros((2 * NT, BLOCK), BF16)
    for s in range(STEPS):
        owns[s][RB] = zero_block

    @pl.when(lat == 0)
    def _():
        for s in range(STEPS):
            rims[s][0][...] = jnp.zeros((HB, 2 * NT, BLOCK), BF16)

    @pl.when(lat == N_LAT - 1)
    def _():
        for s in range(STEPS):
            rims[s][1][...] = jnp.zeros((HB, 2 * NT, BLOCK), BF16)

    loads[0].wait()
    loads[1].wait()
    loads[2].wait()
    for b in range(RB):
        own_0[b] = jnp.concatenate([state0[:, cols(b)], tang0[:, cols(b)]], axis=0).astype(BF16)

    for d in range(4):
        for h in range(HB):
            picks[0, d, h] = own_0[sends[0, h, d]]
    pl.semaphore_wait(barrier, 4 + lat_count + z_count(1))
    send_lat_rims(0)
    send_lon_rims(0)
    tell(0)

    crow_copies = [
        pltpu.make_async_remote_copy(
            src_ref=crow_own,
            dst_ref=crow_side.at[i],
            send_sem=crow_send,
            recv_sem=crow_recv,
            device_id=lon_at(step),
            device_id_type=MESH,
        )
        for i, step in enumerate((1, -1))
    ]

    def group(ref, send_sem, recv_sem):
        return pltpu.make_async_remote_copy(
            src_ref=ref,
            dst_ref=ref,
            send_sem=send_sem,
            recv_sem=recv_sem,
            device_id=lon_at(1),
            device_id_type=MESH,
        )

    crow_all = group(crow_side, crow_send, crow_recv)

    for i in range(3, 9):
        loads[i].wait()

    lane16 = lax.broadcasted_iota(jnp.int32, (NT, BLOCK), 1)
    row16 = lax.broadcasted_iota(jnp.int32, (NT, BLOCK), 0)
    spread = (lane16 % NT == row16).astype(F32)
    tiled = STEP_LENGTH * jnp.dot(
        coup[...], spread, precision=lax.Precision.HIGHEST, preferred_element_type=F32
    )
    tiled = jnp.concatenate([tiled, tiled], axis=0)
    lane32 = lax.broadcasted_iota(jnp.int32, (2 * NT, BLOCK), 1)
    row32 = lax.broadcasted_iota(jnp.int32, (2 * NT, BLOCK), 0)
    tiled_hi = tiled.astype(BF16).astype(F32)
    tiled_part = jnp.where(lane32 < 64, tiled_hi, tiled - tiled_hi)
    mixer = jnp.where((lane32 % 32) // NT == row32 // NT, tiled_part, 0.0).astype(BF16)

    local_region = region[...] - lat * (N_LON * REG_DEV)
    region_t = jnp.transpose(
        jnp.concatenate([local_region.astype(F32)] * (BLOCK // RB), axis=0), (1, 0)
    )

    def own_part(s):
        for b in range(RB):
            if s == 0:
                st, tg = state0[:, cols(b)], tang0[:, cols(b)]
            else:
                st, tg = stk[b, :NT], stk[b, NT:]
            squared = st * st
            inverse = 1.0 / (1.0 + squared)
            scaled = rate[b : b + 1, :] * inverse
            uptake = scaled * st
            slope = scaled * (1.0 - squared) * inverse * tg
            both = jnp.concatenate([uptake, slope], axis=0)
            both_hi = both.astype(BF16)
            both_lo = (both - both_hi.astype(F32)).astype(BF16)
            sources = jnp.dot(
                mixer,
                jnp.concatenate([both_hi, both_lo, both_hi, both_lo], axis=0),
                preferred_element_type=F32,
            )
            extra = lists[K - 1, b]
            extra = jnp.where(extra >= RB, RB, extra)
            gathered = jnp.concatenate([owns[s][b], owns[s][extra]], axis=1)
            weights = jnp.concatenate([coef[b, 0], coef[b, K - 1]], axis=0)
            moved = jnp.dot(gathered, weights, preferred_element_type=F32)
            acc[b] = jnp.concatenate([st, tg], axis=0) + (moved + sources)

    def explicit_of(s, b):
        parts = [rims[s][d][lists[1 + d, b] % HB] for d in range(4)]
        gathered = jnp.concatenate(parts, axis=1)
        weights = coef[b, 1:5].reshape(4 * BLOCK, BLOCK)
        moved = jnp.dot(gathered, weights, preferred_element_type=F32)
        return (acc[b] + moved).astype(BF16)

    def rim_part(s):
        for b in range(RB):
            explicit[b] = explicit_of(s, b)

    def implicit_part(b):
        return jnp.dot(explicit[b], impl[b], preferred_element_type=F32)

    own_part(0)
    loads[9].wait()
    for copy in crow_copies:
        copy.start()
    hear(0)
    tell(1)
    await_rims(0)
    await_rim_sends(0)
    for first, send in ((0, send_lat_rims), (2, send_lon_rims)):
        order = [(d, h, sends[0, h, d]) for d in (first, first + 1) for h in range(HB)]
        for d, h, b in order:
            explicit[d * HB + h] = explicit_of(0, b)
        for d, h, b in order:
            made = jnp.dot(explicit[d * HB + h], impl[b], preferred_element_type=F32)
            picks[1, d, h] = made.astype(BF16)
        send(1)
    hear(1)
    tell(2)
    rim_part(0)
    for b in range(RB):
        new = implicit_part(b)
        stk[b] = new
        own_1[b] = new.astype(BF16)
    own_part(1)

    lanes = lax.broadcasted_iota(jnp.int32, (BLOCK, BLOCK), 1).astype(F32)
    first = (lat * N_LON + lon - 1) * REG_DEV
    slot = (region[...] - first) & (N_LON * REG_DEV - 1)
    rows = lax.broadcasted_iota(jnp.int32, (BLOCK, BLOCK), 0) % 32
    for b in range(RB):
        onehot_t[b] = jnp.where(region_t[:, b : b + 1] == lanes, 1.0, 0.0).astype(BF16)
        onehot[:, cols(b)] = jnp.where(rows == slot[b : b + 1, :], 1.0, 0.0).astype(BF16)

    for b in range(RB):
        folded[b] = jnp.dot(impl[b], onehot_t[b], preferred_element_type=F32).astype(BF16)
    partial = jnp.zeros((NT, BLOCK), F32)
    for b in range(RB):
        partial += jnp.dot(
            jnp.concatenate([acc[b, NT:].astype(BF16), -own_0[b, NT:]], axis=1),
            jnp.concatenate([folded[b], onehot_t[b]], axis=0),
            preferred_element_type=F32,
        )
    for d in range(4):
        both = jnp.zeros((BLOCK, BLOCK), F32)
        second = jnp.zeros((BLOCK, BLOCK), F32)
        for b in range(RB):
            product = jnp.dot(coef[b, 1 + d], folded[b], preferred_element_type=F32)
            both += product
            second += product * (lists[1 + d, b] % HB).astype(F32)
        rim_w[HB * d] = (both - second).astype(BF16)
        rim_w[HB * d + 1] = second.astype(BF16)

    await_rims(1)
    tangents = [rims[1][d][h, NT:] for d in range(4) for h in range(HB)]
    partial += jnp.dot(
        jnp.concatenate(tangents, axis=1),
        rim_w[...].reshape(4 * HB * BLOCK, BLOCK),
        preferred_element_type=F32,
    )
    tile_lon[...] = partial.astype(BF16)

    hear(2)
    tell(3)
    for i, p in enumerate(LON_PEERS):
        pltpu.make_async_remote_copy(
            src_ref=tile_lon,
            dst_ref=lon_buf.at[i],
            send_sem=lon_send,
            recv_sem=lon_recv,
            device_id=lon_peer(*p),
            device_id_type=MESH,
        ).start()

    rim_part(1)
    for b in range(RB):
        new = implicit_part(b)
        state_out[:, cols(b)] = new[:NT]
        precond_out[:, cols(b)] = new[NT:] - tang0[:, cols(b)]

    crow_all.wait_recv()
    zero_rows = jnp.zeros((REG_DEV, BLOCK), F32)
    for k in range(NZ):
        parts = []
        for i in range(NX):
            at = cols(k * NX + i)
            parts += [crow_side[0, :, at], crow_own[:, at], crow_side[1, :, at], zero_rows]
        coarse_w[k] = jnp.transpose(jnp.concatenate(parts, axis=0), (1, 0)).astype(BF16)

    totals = partial.astype(BF16).astype(F32)
    lon_all = group(lon_buf, lon_send, lon_recv)
    lon_all.wait_recv()
    for i in range(len(LON_PEERS)):
        totals += lon_buf[i].astype(F32)
    tile_lat[...] = totals.astype(BF16)
    lat_buf[lat] = totals.astype(BF16)

    hear(3)
    for i in range(N_LAT - 1):
        peer = jnp.where(lat <= i, i + 1, i)
        pltpu.make_async_remote_copy(
            src_ref=tile_lat,
            dst_ref=lat_buf.at[lat],
            send_sem=lat_send,
            recv_sem=lat_recv,
            device_id=at_lat(peer),
            device_id_type=MESH,
        ).start()
    crow_all.wait_send()
    lon_all.wait_send()
    await_rim_sends(1)
    lat_all = group(lat_buf.at[pl.ds(0, N_LAT - 1)], lat_send, lat_recv)
    lat_all.wait_recv()

    tiles = [lat_buf[NX * k : NX * (k + 1)].reshape(NX * NT, BLOCK) for k in range(NZ)]
    values = jnp.dot(
        jnp.concatenate(tiles, axis=1),
        coarse_w[...].reshape(NZ * BLOCK, BLOCK),
        preferred_element_type=F32,
    )
    own_values = jnp.where(lane16 // 32 == 0, values[:NT], 0.0)
    for i in range(1, NX):
        own_values += jnp.where(lane16 // 32 == i, values[i * NT : (i + 1) * NT], 0.0)
    high = own_values.astype(BF16)
    low = (own_values - high.astype(F32)).astype(BF16)
    spread_values = jnp.dot(
        jnp.concatenate([high, low], axis=0), onehot[...], preferred_element_type=F32
    )
    precond_out[...] += spread_values[:NT] + spread_values[NT:]
    lat_all.wait_send()


def write_kernel(state_ref, precond_ref, state_out, precond_out, sem):
    copies = [
        pltpu.make_async_copy(state_ref, state_out, sem.at[0]),
        pltpu.make_async_copy(precond_ref, precond_out, sem.at[1]),
    ]
    for copy in copies:
        copy.start()
    for copy in copies:
        copy.wait()


def local(
    state_init,
    tangent_init,
    coef_blocks,
    column_lists,
    send_lists,
    implicit_blocks,
    uptake_rate,
    coupling,
    region_map,
    coarse_inverse,
):
    rows = RB * BLOCK
    hbm_spec = pl.BlockSpec(memory_space=pltpu.HBM)
    vmem_spec = pl.BlockSpec(memory_space=pltpu.VMEM)
    rim = pltpu.VMEM((HB, 2 * NT, BLOCK), BF16)
    outs = (
        jax.ShapeDtypeStruct((NT, rows), F32),
        jax.ShapeDtypeStruct((NT, rows), F32),
    )
    results = pl.pallas_call(
        kernel,
        name="tracer_step",
        out_shape=outs,
        in_specs=[hbm_spec] * 10,
        out_specs=(vmem_spec, vmem_spec),
        scratch_shapes=[
            pltpu.VMEM((NT, rows), F32),
            pltpu.VMEM((NT, rows), F32),
            pltpu.VMEM((RB, K, BLOCK, BLOCK), BF16),
            pltpu.VMEM((RB, BLOCK, BLOCK), BF16),
            pltpu.VMEM((RB, BLOCK), F32),
            pltpu.VMEM((NT, NT), F32),
            pltpu.VMEM((RB, BLOCK), jnp.int32),
            pltpu.VMEM((REG_DEV, N_LAT * BLOCK), F32),
            pltpu.VMEM((2, REG_DEV, N_LAT * BLOCK), F32),
            pltpu.SMEM((K, RB), jnp.int32),
            pltpu.SMEM((1, HB, 4), jnp.int32),
            pltpu.VMEM((RB + 1, 2 * NT, BLOCK), BF16),
            pltpu.VMEM((RB + 1, 2 * NT, BLOCK), BF16),
            rim,
            rim,
            rim,
            rim,
            rim,
            rim,
            rim,
            rim,
            pltpu.VMEM((STEPS, 4, HB, 2 * NT, BLOCK), BF16),
            pltpu.VMEM((RB, 2 * NT, BLOCK), F32),
            pltpu.VMEM((RB, 2 * NT, BLOCK), BF16),
            pltpu.VMEM((RB, BLOCK, BLOCK), BF16),
            pltpu.VMEM((4 * HB, BLOCK, BLOCK), BF16),
            pltpu.VMEM((RB, 2 * NT, BLOCK), F32),
            pltpu.VMEM((RB, BLOCK, BLOCK), BF16),
            pltpu.VMEM((BLOCK, rows), BF16),
            pltpu.VMEM((NZ, BLOCK, BLOCK), BF16),
            pltpu.VMEM((NT, BLOCK), BF16),
            pltpu.VMEM((len(LON_PEERS), NT, BLOCK), BF16),
            pltpu.VMEM((NT, BLOCK), BF16),
            pltpu.VMEM((N_LAT, NT, BLOCK), BF16),
            pltpu.SemaphoreType.DMA((10,)),
            pltpu.SemaphoreType.DMA((4,)),
            pltpu.SemaphoreType.DMA((STEPS, 4)),
            pltpu.SemaphoreType.DMA,
            pltpu.SemaphoreType.DMA,
            pltpu.SemaphoreType.DMA,
            pltpu.SemaphoreType.DMA,
            pltpu.SemaphoreType.DMA,
            pltpu.SemaphoreType.DMA,
            pltpu.SemaphoreType.REGULAR((4,)),
        ],
        compiler_params=pltpu.CompilerParams(
            collective_id=0, has_side_effects=True, vmem_limit_bytes=24 * 2**20
        ),
    )(
        *(
            pltpu.with_memory_space_constraint(value, pltpu.HBM)
            for value in (
                state_init,
                tangent_init,
                coef_blocks,
                column_lists.T,
                send_lists.transpose(0, 2, 1),
                implicit_blocks,
                uptake_rate.reshape(RB, BLOCK),
                coupling,
                region_map.reshape(RB, BLOCK),
                coarse_inverse,
            )
        )
    )
    return pl.pallas_call(
        write_kernel,
        name="write_out",
        out_shape=outs,
        in_specs=[vmem_spec, vmem_spec],
        out_specs=(hbm_spec, hbm_spec),
        scratch_shapes=[pltpu.SemaphoreType.DMA((2,))],
        compiler_params=pltpu.CompilerParams(vmem_limit_bytes=4 * 2**20),
    )(*results)


def solution(mesh):
    torus = Mesh(mesh.devices.reshape(NZ, NX, NY, NCORE), AXES)
    placed = (
        P(None, AXES),
        P(None, AXES),
        P(AXES, None, None, None),
        P(AXES, None),
        P(AXES, None, None),
        P(AXES, None, None),
        P(AXES),
        P(),
        P(AXES),
        P(AXES, None),
    )
    return jax.shard_map(
        local,
        mesh=torus,
        in_specs=placed,
        out_specs=(P(None, AXES), P(None, AXES)),
        check_vma=False,
    )
```

```python
import jax
import jax.numpy as jnp
from jax import lax
from jax.experimental import pallas as pl
from jax.experimental.pallas import tpu as pltpu
from jax.sharding import Mesh
from jax.sharding import PartitionSpec as P

NT = 16
STEPS = 2
REG_DEV = 8
RB = 16
K = 6
HB = 2
BLOCK = 128
STEP_LENGTH = 0.5
AXES = ("z", "x", "y", "c")
NZ, NX, NY, NCORE = 8, 4, 8, 2
N_LAT = NZ * NX
N_LON = NY * NCORE
MESH = pl.DeviceIdType.MESH
F32 = jnp.float32
BF16 = jnp.bfloat16


def ring_hops(d, n):
    return min(d, n - d)


LON_PEERS = sorted(
    ((dy, dc) for dy in range(NY) for dc in range(NCORE) if (dy, dc) != (0, 0)),
    key=lambda p: -ring_hops(p[0], NY),
)

def kernel(
    state_hbm,
    tangent_hbm,
    coef_hbm,
    lists_hbm,
    sends_hbm,
    implicit_hbm,
    rate_hbm,
    coupling_hbm,
    region_hbm,
    coarse_hbm,
    state_out,
    precond_out,
    state0,
    tang0,
    coef,
    impl,
    rate,
    coup,
    region,
    crow_own,
    crow_side,
    lists,
    sends,
    own_0,
    own_1,
    rims_0,
    rims_1,
    rims_2,
    rims_3,
    rims_4,
    rims_5,
    rims_6,
    rims_7,
    picks,
    acc,
    explicit,
    folded,
    rim_w,
    stk,
    onehot_t,
    onehot,
    coarse_w,
    tile_lon,
    lon_buf,
    tile_lat,
    lat_buf,
    load_sem,
    rim_send,
    rim_recv,
    crow_send,
    crow_recv,
    lon_send,
    lon_recv,
    lat_send,
    lat_recv,
    known,
):
    z, x = lax.axis_index("z"), lax.axis_index("x")
    y, c = lax.axis_index("y"), lax.axis_index("c")
    lat = z * NX + x
    lon = y * NCORE + c
    owns = (own_0, own_1)
    rims = ((rims_0, rims_1, rims_2, rims_3), (rims_4, rims_5, rims_6, rims_7))

    def at_lat(v):
        return (v // NX, v % NX, y, c)

    def at_lon(v):
        return (z, x, v // NCORE, v % NCORE)

    def lon_peer(dy, dc):
        return (z, x, (y + dy) % NY, (c + dc) % NCORE)

    def torus_at(dz, dx):
        return ((z + dz) % NZ, (x + dx) % NX, y, c)

    pairs = (
        (sends_hbm, sends),
        (state_hbm, state0),
        (tangent_hbm, tang0),
        (lists_hbm, lists),
        (rate_hbm, rate),
        (coupling_hbm, coup),
        (region_hbm, region),
        (coef_hbm, coef),
        (implicit_hbm, impl),
        (coarse_hbm, crow_own),
    )
    loads = [pltpu.make_async_copy(a, b, load_sem.at[i]) for i, (a, b) in enumerate(pairs)]
    loads[0].start()
    half = RB * BLOCK // 2
    for i in (1, 2):
        for row in (0, NT // 2):
            for col in (0, half):
                piece = (slice(row, row + NT // 2), slice(col, col + half))
                pltpu.make_async_copy(
                    pairs[i][0].at[piece], pairs[i][1].at[piece], load_sem.at[i]
                ).start()
    for load in loads[3:]:
        load.start()

    def signal(sem, peer):
        pl.semaphore_signal(sem, inc=1, device_id=peer, device_id_type=MESH)

    def lon_at(step):
        return at_lon((lon + step + N_LON) % N_LON)

    def z_at(step):
        return torus_at(step + NZ, 0)

    def x_at(step):
        return torus_at(0, step + NX)

    def signal_z(sem, reach):
        @pl.when(z + reach < NZ)
        def _():
            signal(sem, z_at(reach))

        @pl.when(z >= reach)
        def _():
            signal(sem, z_at(-reach))

    def z_count(reach):
        return jnp.where(z + reach < NZ, 1, 0) + jnp.where(z >= reach, 1, 0)

    barrier = pltpu.get_barrier_semaphore()

    @pl.when(lat < N_LAT - 1)
    def _():
        signal(barrier, at_lat(lat + 1))

    @pl.when(lat > 0)
    def _():
        signal(barrier, at_lat(lat - 1))

    for step in (1, -1):
        signal(barrier, lon_at(step))
        signal(barrier, x_at(step))
    signal_z(barrier, 1)
    lat_count = jnp.where(lat < N_LAT - 1, 1, 0) + jnp.where(lat > 0, 1, 0)

    def tell(stage):
        sem = known.at[stage]
        if stage < 3:
            signal(sem, lon_at(2**stage))
            signal(sem, lon_at(-(2**stage)))
        if stage == 0:
            signal(sem, x_at(1))
            signal(sem, x_at(-1))
        if stage < 2:
            signal_z(sem, 2**stage)
        elif stage == 2:
            signal(sem, z_at(4))
        else:
            for i in range(1, NX):
                signal(sem, x_at(i))

    def hear(stage):
        counts = (4 + z_count(1), 2 + z_count(2), 3, NX - 1)
        pl.semaphore_wait(known.at[stage], counts[stage])

    def cols(b):
        return slice(b * BLOCK, (b + 1) * BLOCK)

    def rim_copies(s):
        below, above = (lat + N_LAT - 1) % N_LAT, (lat + 1) % N_LAT
        west, east = (lon + N_LON - 1) % N_LON, (lon + 1) % N_LON
        targets = (at_lat(above), at_lat(below), at_lon(east), at_lon(west))
        return [
            pltpu.make_async_remote_copy(
                src_ref=picks.at[s, d],
                dst_ref=rims[s][d],
                send_sem=rim_send.at[d],
                recv_sem=rim_recv.at[s, d],
                device_id=targets[d],
                device_id_type=MESH,
            )
            for d in range(4)
        ]

    def send_lat_rims(s):
        copies = rim_copies(s)

        @pl.when(lat < N_LAT - 1)
        def _():
            copies[0].start()

        @pl.when(lat > 0)
        def _():
            copies[1].start()

    def send_lon_rims(s):
        copies = rim_copies(s)
        copies[2].start()
        copies[3].start()

    def await_rims(s):
        copies = rim_copies(s)

        @pl.when(lat > 0)
        def _():
            copies[0].wait_recv()

        @pl.when(lat < N_LAT - 1)
        def _():
            copies[1].wait_recv()

        copies[2].wait_recv()
        copies[3].wait_recv()

    def await_rim_sends(s):
        copies = rim_copies(s)

        @pl.when(lat < N_LAT - 1)
        def _():
            copies[0].wait_send()

        @pl.when(lat > 0)
        def _():
            copies[1].wait_send()

        copies[2].wait_send()
        copies[3].wait_send()

    zero_block = jnp.zeros((2 * NT, BLOCK), BF16)
    for s in range(STEPS):
        owns[s][RB] = zero_block

    @pl.when(lat == 0)
    def _():
        for s in range(STEPS):
            rims[s][0][...] = jnp.zeros((HB, 2 * NT, BLOCK), BF16)

    @pl.when(lat == N_LAT - 1)
    def _():
        for s in range(STEPS):
            rims[s][1][...] = jnp.zeros((HB, 2 * NT, BLOCK), BF16)

    loads[0].wait()
    loads[1].wait()
    loads[2].wait()
    for b in range(RB):
        own_0[b] = jnp.concatenate([state0[:, cols(b)], tang0[:, cols(b)]], axis=0).astype(BF16)

    for d in range(4):
        for h in range(HB):
            picks[0, d, h] = own_0[sends[0, h, d]]
    pl.semaphore_wait(barrier, 4 + lat_count + z_count(1))
    send_lat_rims(0)
    send_lon_rims(0)
    tell(0)

    crow_copies = [
        pltpu.make_async_remote_copy(
            src_ref=crow_own,
            dst_ref=crow_side.at[i],
            send_sem=crow_send,
            recv_sem=crow_recv,
            device_id=lon_at(step),
            device_id_type=MESH,
        )
        for i, step in enumerate((1, -1))
    ]

    def group(ref, send_sem, recv_sem):
        return pltpu.make_async_remote_copy(
            src_ref=ref,
            dst_ref=ref,
            send_sem=send_sem,
            recv_sem=recv_sem,
            device_id=lon_at(1),
            device_id_type=MESH,
        )

    crow_all = group(crow_side, crow_send, crow_recv)

    for i in range(3, 9):
        loads[i].wait()

    lane16 = lax.broadcasted_iota(jnp.int32, (NT, BLOCK), 1)
    row16 = lax.broadcasted_iota(jnp.int32, (NT, BLOCK), 0)
    spread = (lane16 % NT == row16).astype(F32)
    tiled = STEP_LENGTH * jnp.dot(
        coup[...], spread, precision=lax.Precision.HIGHEST, preferred_element_type=F32
    )
    tiled = jnp.concatenate([tiled, tiled], axis=0)
    lane32 = lax.broadcasted_iota(jnp.int32, (2 * NT, BLOCK), 1)
    row32 = lax.broadcasted_iota(jnp.int32, (2 * NT, BLOCK), 0)
    tiled_hi = tiled.astype(BF16).astype(F32)
    tiled_part = jnp.where(lane32 < 64, tiled_hi, tiled - tiled_hi)
    mixer = jnp.where((lane32 % 32) // NT == row32 // NT, tiled_part, 0.0).astype(BF16)

    local_region = region[...] - lat * (N_LON * REG_DEV)
    region_t = jnp.transpose(
        jnp.concatenate([local_region.astype(F32)] * (BLOCK // RB), axis=0), (1, 0)
    )

    def own_part(s):
        for b in range(RB):
            if s == 0:
                st, tg = state0[:, cols(b)], tang0[:, cols(b)]
            else:
                st, tg = stk[b, :NT], stk[b, NT:]
            squared = st * st
            inverse = 1.0 / (1.0 + squared)
            scaled = rate[b : b + 1, :] * inverse
            uptake = scaled * st
            slope = scaled * (1.0 - squared) * inverse * tg
            both = jnp.concatenate([uptake, slope], axis=0)
            both_hi = both.astype(BF16)
            both_lo = (both - both_hi.astype(F32)).astype(BF16)
            sources = jnp.dot(
                mixer,
                jnp.concatenate([both_hi, both_lo, both_hi, both_lo], axis=0),
                preferred_element_type=F32,
            )
            extra = lists[K - 1, b]
            extra = jnp.where(extra >= RB, RB, extra)
            gathered = jnp.concatenate([owns[s][b], owns[s][extra]], axis=1)
            weights = jnp.concatenate([coef[b, 0], coef[b, K - 1]], axis=0)
            moved = jnp.dot(gathered, weights, preferred_element_type=F32)
            acc[b] = jnp.concatenate([st, tg], axis=0) + (moved + sources)

    def explicit_of(s, b):
        parts = [rims[s][d][lists[1 + d, b] % HB] for d in range(4)]
        gathered = jnp.concatenate(parts, axis=1)
        weights = coef[b, 1:5].reshape(4 * BLOCK, BLOCK)
        moved = jnp.dot(gathered, weights, preferred_element_type=F32)
        return (acc[b] + moved).astype(BF16)

    def rim_part(s):
        for b in range(RB):
            explicit[b] = explicit_of(s, b)

    def implicit_part(b):
        return jnp.dot(explicit[b], impl[b], preferred_element_type=F32)

    own_part(0)
    loads[9].wait()
    for copy in crow_copies:
        copy.start()
    hear(0)
    tell(1)
    await_rims(0)
    await_rim_sends(0)
    for first, send in ((0, send_lat_rims), (2, send_lon_rims)):
        order = [(d, h, sends[0, h, d]) for d in (first, first + 1) for h in range(HB)]
        for d, h, b in order:
            explicit[d * HB + h] = explicit_of(0, b)
        for d, h, b in order:
            made = jnp.dot(explicit[d * HB + h], impl[b], preferred_element_type=F32)
            picks[1, d, h] = made.astype(BF16)
        send(1)
    hear(1)
    tell(2)
    rim_part(0)
    for b in range(RB):
        new = implicit_part(b)
        stk[b] = new
        own_1[b] = new.astype(BF16)
    own_part(1)

    lanes = lax.broadcasted_iota(jnp.int32, (BLOCK, BLOCK), 1).astype(F32)
    first = (lat * N_LON + lon - 1) * REG_DEV
    slot = (region[...] - first) & (N_LON * REG_DEV - 1)
    rows = lax.broadcasted_iota(jnp.int32, (BLOCK, BLOCK), 0) % 32
    for b in range(RB):
        onehot_t[b] = jnp.where(region_t[:, b : b + 1] == lanes, 1.0, 0.0).astype(BF16)
        onehot[:, cols(b)] = jnp.where(rows == slot[b : b + 1, :], 1.0, 0.0).astype(BF16)

    for b in range(RB):
        folded[b] = jnp.dot(impl[b], onehot_t[b], preferred_element_type=F32).astype(BF16)
    partial = jnp.zeros((NT, BLOCK), F32)
    for b in range(RB):
        partial += jnp.dot(
            jnp.concatenate([acc[b, NT:].astype(BF16), -own_0[b, NT:]], axis=1),
            jnp.concatenate([folded[b], onehot_t[b]], axis=0),
            preferred_element_type=F32,
        )
    for d in range(4):
        both = jnp.zeros((BLOCK, BLOCK), F32)
        second = jnp.zeros((BLOCK, BLOCK), F32)
        for b in range(RB):
            product = jnp.dot(coef[b, 1 + d], folded[b], preferred_element_type=F32)
            both += product
            second += product * (lists[1 + d, b] % HB).astype(F32)
        rim_w[HB * d] = (both - second).astype(BF16)
        rim_w[HB * d + 1] = second.astype(BF16)

    await_rims(1)
    tangents = [rims[1][d][h, NT:] for d in range(4) for h in range(HB)]
    partial += jnp.dot(
        jnp.concatenate(tangents, axis=1),
        rim_w[...].reshape(4 * HB * BLOCK, BLOCK),
        preferred_element_type=F32,
    )
    tile_lon[...] = partial.astype(BF16)

    hear(2)
    for i, p in enumerate(LON_PEERS):
        pltpu.make_async_remote_copy(
            src_ref=tile_lon,
            dst_ref=lon_buf.at[i],
            send_sem=lon_send,
            recv_sem=lon_recv,
            device_id=lon_peer(*p),
            device_id_type=MESH,
        ).start()

    tell(3)
    rim_part(1)
    for b in range(RB):
        new = implicit_part(b)
        state_out[:, cols(b)] = new[:NT]
        precond_out[:, cols(b)] = new[NT:] - tang0[:, cols(b)]

    crow_all.wait_recv()
    zero_rows = jnp.zeros((REG_DEV, BLOCK), F32)
    for k in range(NZ):
        parts = []
        for i in range(NX):
            at = cols(k * NX + i)
            parts += [crow_side[0, :, at], crow_own[:, at], crow_side[1, :, at], zero_rows]
        coarse_w[k] = jnp.transpose(jnp.concatenate(parts, axis=0), (1, 0)).astype(BF16)

    totals = partial.astype(BF16).astype(F32)
    lon_all = group(lon_buf, lon_send, lon_recv)
    lon_all.wait_recv()
    for i in range(len(LON_PEERS)):
        totals += lon_buf[i].astype(F32)
    tile_lat[...] = totals.astype(BF16)
    lat_buf[lat] = totals.astype(BF16)

    hear(3)
    for i in range(N_LAT - 1):
        peer = jnp.where(lat <= i, i + 1, i)
        pltpu.make_async_remote_copy(
            src_ref=tile_lat,
            dst_ref=lat_buf.at[lat],
            send_sem=lat_send,
            recv_sem=lat_recv,
            device_id=at_lat(peer),
            device_id_type=MESH,
        ).start()
    crow_all.wait_send()
    lon_all.wait_send()
    await_rim_sends(1)
    lat_all = group(lat_buf.at[pl.ds(0, N_LAT - 1)], lat_send, lat_recv)
    lat_all.wait_recv()

    tiles = [lat_buf[NX * k : NX * (k + 1)].reshape(NX * NT, BLOCK) for k in range(NZ)]
    values = jnp.dot(
        jnp.concatenate(tiles, axis=1),
        coarse_w[...].reshape(NZ * BLOCK, BLOCK),
        preferred_element_type=F32,
    )
    own_values = jnp.where(lane16 // 32 == 0, values[:NT], 0.0)
    for i in range(1, NX):
        own_values += jnp.where(lane16 // 32 == i, values[i * NT : (i + 1) * NT], 0.0)
    high = own_values.astype(BF16)
    low = (own_values - high.astype(F32)).astype(BF16)
    spread_values = jnp.dot(
        jnp.concatenate([high, low], axis=0), onehot[...], preferred_element_type=F32
    )
    precond_out[...] += spread_values[:NT] + spread_values[NT:]
    lat_all.wait_send()


def write_kernel(state_ref, precond_ref, state_out, precond_out, sem):
    copies = [
        pltpu.make_async_copy(state_ref, state_out, sem.at[0]),
        pltpu.make_async_copy(precond_ref, precond_out, sem.at[1]),
    ]
    for copy in copies:
        copy.start()
    for copy in copies:
        copy.wait()


def local(
    state_init,
    tangent_init,
    coef_blocks,
    column_lists,
    send_lists,
    implicit_blocks,
    uptake_rate,
    coupling,
    region_map,
    coarse_inverse,
):
    rows = RB * BLOCK
    hbm_spec = pl.BlockSpec(memory_space=pltpu.HBM)
    vmem_spec = pl.BlockSpec(memory_space=pltpu.VMEM)
    rim = pltpu.VMEM((HB, 2 * NT, BLOCK), BF16)
    outs = (
        jax.ShapeDtypeStruct((NT, rows), F32),
        jax.ShapeDtypeStruct((NT, rows), F32),
    )
    results = pl.pallas_call(
        kernel,
        name="tracer_step",
        out_shape=outs,
        in_specs=[hbm_spec] * 10,
        out_specs=(vmem_spec, vmem_spec),
        scratch_shapes=[
            pltpu.VMEM((NT, rows), F32),
            pltpu.VMEM((NT, rows), F32),
            pltpu.VMEM((RB, K, BLOCK, BLOCK), BF16),
            pltpu.VMEM((RB, BLOCK, BLOCK), BF16),
            pltpu.VMEM((RB, BLOCK), F32),
            pltpu.VMEM((NT, NT), F32),
            pltpu.VMEM((RB, BLOCK), jnp.int32),
            pltpu.VMEM((REG_DEV, N_LAT * BLOCK), F32),
            pltpu.VMEM((2, REG_DEV, N_LAT * BLOCK), F32),
            pltpu.SMEM((K, RB), jnp.int32),
            pltpu.SMEM((1, HB, 4), jnp.int32),
            pltpu.VMEM((RB + 1, 2 * NT, BLOCK), BF16),
            pltpu.VMEM((RB + 1, 2 * NT, BLOCK), BF16),
            rim,
            rim,
            rim,
            rim,
            rim,
            rim,
            rim,
            rim,
            pltpu.VMEM((STEPS, 4, HB, 2 * NT, BLOCK), BF16),
            pltpu.VMEM((RB, 2 * NT, BLOCK), F32),
            pltpu.VMEM((RB, 2 * NT, BLOCK), BF16),
            pltpu.VMEM((RB, BLOCK, BLOCK), BF16),
            pltpu.VMEM((4 * HB, BLOCK, BLOCK), BF16),
            pltpu.VMEM((RB, 2 * NT, BLOCK), F32),
            pltpu.VMEM((RB, BLOCK, BLOCK), BF16),
            pltpu.VMEM((BLOCK, rows), BF16),
            pltpu.VMEM((NZ, BLOCK, BLOCK), BF16),
            pltpu.VMEM((NT, BLOCK), BF16),
            pltpu.VMEM((len(LON_PEERS), NT, BLOCK), BF16),
            pltpu.VMEM((NT, BLOCK), BF16),
            pltpu.VMEM((N_LAT, NT, BLOCK), BF16),
            pltpu.SemaphoreType.DMA((10,)),
            pltpu.SemaphoreType.DMA((4,)),
            pltpu.SemaphoreType.DMA((STEPS, 4)),
            pltpu.SemaphoreType.DMA,
            pltpu.SemaphoreType.DMA,
            pltpu.SemaphoreType.DMA,
            pltpu.SemaphoreType.DMA,
            pltpu.SemaphoreType.DMA,
            pltpu.SemaphoreType.DMA,
            pltpu.SemaphoreType.REGULAR((4,)),
        ],
        compiler_params=pltpu.CompilerParams(
            collective_id=0, has_side_effects=True, vmem_limit_bytes=24 * 2**20
        ),
    )(
        *(
            pltpu.with_memory_space_constraint(value, pltpu.HBM)
            for value in (
                state_init,
                tangent_init,
                coef_blocks,
                column_lists.T,
                send_lists.transpose(0, 2, 1),
                implicit_blocks,
                uptake_rate.reshape(RB, BLOCK),
                coupling,
                region_map.reshape(RB, BLOCK),
                coarse_inverse,
            )
        )
    )
    return pl.pallas_call(
        write_kernel,
        name="write_out",
        out_shape=outs,
        in_specs=[vmem_spec, vmem_spec],
        out_specs=(hbm_spec, hbm_spec),
        scratch_shapes=[pltpu.SemaphoreType.DMA((2,))],
        compiler_params=pltpu.CompilerParams(vmem_limit_bytes=4 * 2**20),
    )(*results)


def solution(mesh):
    torus = Mesh(mesh.devices.reshape(NZ, NX, NY, NCORE), AXES)
    placed = (
        P(None, AXES),
        P(None, AXES),
        P(AXES, None, None, None),
        P(AXES, None),
        P(AXES, None, None),
        P(AXES, None, None),
        P(AXES),
        P(),
        P(AXES),
        P(AXES, None),
    )
    return jax.shard_map(
        local,
        mesh=torus,
        in_specs=placed,
        out_specs=(P(None, AXES), P(None, AXES)),
        check_vma=False,
    )
```
